256 devices in a mesh: row: 8 (over y, core), col: 32 (over x, z).
Axes of the slice: x: 4, y: 4, z: 8, core: 2. Of those that a mesh axis runs over, the one named last changes fastest.
Arguments:
- eigvecs: float32 [1024, 100352], P('col', 'row'), may hold values from -6 to 6
- span_vectors: float32 [2, 64, 4, 128], P(None, 'row'), may hold values from -6 to 6
- span_offsets: int32 [2, 64], P(None, 'row'), may hold values from 0 to 12543, as said below
- panels: bfloat16 [2, 256, 100352], P(None, 'col', 'row'), may hold values from -0.01894036 to 0.01894036
Outputs:
- back_vectors: float32 [1024, 100352], P('col', 'row')
The draws below stay inside these ranges and needn't reach their ends.
Inputs may be any that keep to these rules, and one draw needn't show every extreme that they name: `span_offsets`: each block starts within the rows of its index of row and ends at most 128 rows after them, and inside the matrix; on every index of row but the last the last block of each sweep reaches into the next index's rows.
All inputs are finite; a program needn't handle non-finite values.
Results may differ from the reference program's by a relative error of at most 0.0075.
Values may be sent and summed in bfloat16 or wider, within the bound.
No kernel may reach another device: no remote copies, remote signals or barrier semaphores. Data moves between devices by JAX's collectives and lax.ppermute only.
A program may use at most 128 MiB of HBM per device.

```python
import jax
import jax.numpy as jnp
from jax import lax

K = 1024
ROWS_DEV = 12544
N = 100352
BAND = 128
REFL = 4
SPANS_DEV = 8
SPANS = 64
SWEEPS = 2
WIDTH = 256
PANELS = 2
N_ROW = 8


def draw_span_offsets(key, part):
    key_base, key_last = jax.random.split(key, 2)
    offsets_all = jax.random.randint(key_base, (SWEEPS, N_ROW, SPANS_DEV), 0, ROWS_DEV - BAND + 1)
    last_span = jax.random.randint(key_last, (SWEEPS, N_ROW), ROWS_DEV - 3 * BAND // 4, ROWS_DEV - BAND // 4 + 1)
    device_ids = jnp.arange(N_ROW)[None, :]
    last_span = jnp.where(device_ids < N_ROW - 1, last_span, ROWS_DEV - BAND)
    offsets_all = offsets_all.at[:, :, SPANS_DEV - 1].set(last_span)
    return offsets_all.reshape(SWEEPS, N_ROW * SPANS_DEV).astype(jnp.int32)


def draw_panels(key, part):
    key_own = jax.random.fold_in(key, 17)
    own = jax.random.truncated_normal(key_own, -4.0, 4.0, (PANELS, WIDTH, N), jnp.float32)
    scaled = own * float(N) ** (-0.5)
    limit = 6.0 * float(N) ** (-0.5)
    return jnp.clip(scaled, -limit, limit).astype(jnp.bfloat16)


def levels(own_key, extent, cuts, least, high):
    def one(axis_at, shards_of):
        heights = jax.random.uniform(jax.random.fold_in(jax.random.fold_in(own_key, 6), axis_at), (shards_of,), jnp.float32, least / len(cuts), high / len(cuts))
        return jnp.repeat(jnp.exp(heights), extent[axis_at] // shards_of).reshape((-1,) + (1,) * (len(extent) - axis_at - 1))

    loudness = one(*cuts[0])
    for cut in cuts[1:]:
        loudness = loudness * one(*cut)
    return loudness


def centred(rng, shape, width, reach, cuts=(), held_as=jnp.bfloat16):
    factor_of = levels(rng, shape, cuts, -0.22, 0.18) if cuts else 1.0
    values = jax.random.normal(rng, shape, jnp.float32) * width * factor_of
    return jnp.minimum(jnp.maximum(values, -reach), reach).astype(held_as)


def setup_inputs(seed: int = 0) -> dict:
    streams_of = jax.random.split(jax.random.key(seed), 5)
    return {
        "eigvecs": centred(streams_of[0], (K, N), 1.0, 6.0, ((0, 32), (1, 8)), jnp.float32),
        "span_vectors": centred(streams_of[1], (SWEEPS, SPANS, REFL, BAND), 1.0, 6.0, ((1, 8),), jnp.float32),
        "span_offsets": draw_span_offsets(jax.random.fold_in(streams_of[4], 71), 0),
        "panels": draw_panels(jax.random.fold_in(streams_of[4], 71), 0),
    }


PRECISE = lax.Precision.HIGHEST
CONTRACT_LAST = (((1,), (1,)), ((), ()))
CONTRACT_FIRST = (((0,), (0,)), ((), ()))

def wy_matrix(gram_mat):
    return jnp.triu(gram_mat, 1) + 0.5 * jnp.diag(jnp.diag(gram_mat))

def apply_span(window, vectors):
    gram_mat = jnp.dot(vectors, vectors.T, precision=PRECISE)
    inner = jnp.dot(vectors, window.T, precision=PRECISE)
    coeffs = lax.linalg.triangular_solve(wy_matrix(gram_mat), inner, left_side=True, lower=False)
    return window - jnp.dot(coeffs.T, vectors, precision=PRECISE)

def reference(eigvecs, span_vectors, span_offsets, panels):
    eigen = eigvecs
    for sweep_at in range(SWEEPS):
        vectors = span_vectors[sweep_at]
        offsets = span_offsets[sweep_at]

        def advance(span_at, state, vectors=vectors, offsets=offsets):
            begin_at = (span_at // SPANS_DEV * ROWS_DEV + offsets[span_at]).astype(jnp.int32)
            window = lax.dynamic_slice_in_dim(state, begin_at, BAND, 1)
            return lax.dynamic_update_slice_in_dim(state, apply_span(window, vectors[span_at]), begin_at, 1)
        eigen = lax.fori_loop(0, SPANS, advance, eigen)
    for panel_at in range(PANELS):
        reflect = panels[panel_at]
        gram_mat = lax.dot_general(reflect.astype(jnp.float32), reflect.astype(jnp.float32), CONTRACT_LAST, preferred_element_type=jnp.float32)
        inner = lax.dot_general(reflect.astype(jnp.float32), eigen.astype(jnp.bfloat16).astype(jnp.float32), CONTRACT_LAST, preferred_element_type=jnp.float32)
        coeffs = lax.linalg.triangular_solve(wy_matrix(gram_mat), inner, left_side=True, lower=False)
        eigen = eigen - lax.dot_general(coeffs.astype(jnp.bfloat16).astype(jnp.float32), reflect.astype(jnp.float32), CONTRACT_FIRST, preferred_element_type=jnp.float32)
    return eigen
```

```python
import functools

import jax
import jax.numpy as jnp
from jax import lax
from jax.experimental import pallas as pl
from jax.experimental.pallas import tpu as pltpu
from jax.sharding import Mesh
from jax.sharding import PartitionSpec as P

COL = ("x", "z")
LANE = 128
F32 = jnp.float32
BF16 = jnp.bfloat16
CONTRACT_LAST = (((1,), (1,)), ((), ()))
HIGH = lax.Precision.HIGHEST


def from_behind(value, axis, steps):
    count = lax.axis_size(axis)
    first, last = (max(0, -steps), min(count, count - steps))
    return lax.ppermute(value, axis, [(source, source + steps) for source in range(first, last)])


def span_factors(vectors):
    refl = len(vectors)
    solved = []
    for i in range(refl):
        value = vectors[i]
        for j in range(i):
            value = value - jnp.sum(vectors[j] * vectors[i], axis=1, keepdims=True) * solved[j]
        pivot = 0.5 * jnp.sum(vectors[i] * vectors[i], axis=1, keepdims=True)
        solved.append(value / pivot)
    return solved


def sweep_body(offsets_ref, vectors_ref, state_ref, pairs_ref):
    spans, refl, band = vectors_ref.shape
    vectors = [vectors_ref[:, i, :] for i in range(refl)]
    factors = span_factors(vectors)
    for i in range(refl):
        pairs_ref[:, i, 0:band] = vectors[i]
        pairs_ref[:, refl + i, 0:band] = factors[i]
        pairs_ref[:, i, band:] = jnp.zeros((spans, band), F32)
        pairs_ref[:, refl + i, band:] = jnp.zeros((spans, band), F32)
    for span_at in range(spans):
        begin = offsets_ref[span_at]
        base = pl.multiple_of(begin // LANE * LANE, LANE)
        moved = pltpu.roll(pairs_ref[span_at], begin - base, 1)
        window = state_ref[:, pl.ds(base, 2 * band)]
        update = window
        for i in range(refl):
            inner = jnp.sum(window * moved[i : i + 1, :], axis=1, keepdims=True)
            update = update - inner * moved[refl + i : refl + i + 1, :]
        state_ref[:, pl.ds(base, 2 * band)] = update


def overhang_kernel(offsets_ref, vectors_ref, own_ref, below_ref, out_ref, state_ref, pairs_ref):
    columns = own_ref.shape[1]
    state_ref[:, 0:columns] = own_ref[...]
    state_ref[:, columns:] = below_ref[...]
    sweep_body(offsets_ref, vectors_ref, state_ref, pairs_ref)
    out_ref[...] = state_ref[:, columns:]


def sweep_kernel(
    place_ref, offsets_ref, vectors_ref, own_ref, above_ref, below_ref, out_ref, *rest, cut
):
    state_ref, pairs_ref = rest[-2:]
    rows, columns = own_ref.shape
    band = below_ref.shape[1]
    state_ref[:, 0:columns] = own_ref[...]
    state_ref[:, columns:] = below_ref[...]

    @pl.when(place_ref[0] > 0)
    def _():
        state_ref[:, 0:band] = above_ref[...]

    sweep_body(offsets_ref, vectors_ref, state_ref, pairs_ref)
    out_ref[...] = state_ref[:, 0:columns]
    if cut:
        pieces_ref = rest[0]
        for at in range(pieces_ref.shape[0]):
            span = min(cut, columns - at * cut)
            pieces_ref[at, :, 0:span] = state_ref[:, at * cut : at * cut + span].astype(BF16)
            if span < cut:
                pieces_ref[at, :, span:] = jnp.zeros((rows, cut - span), BF16)


def sweep_scratch(own, vectors):
    rows, columns = own.shape
    spans, refl, band = vectors.shape
    return [pltpu.VMEM((rows, columns + band), F32), pltpu.VMEM((spans, 2 * refl, 2 * band), F32)]


VM = pl.BlockSpec(memory_space=pltpu.VMEM)
SM = pl.BlockSpec(memory_space=pltpu.SMEM)


def cost(flops, size):
    return pl.CostEstimate(flops=flops, bytes_accessed=size, transcendentals=0)


def overhang(own, below, vectors, offsets):
    return pl.pallas_call(
        overhang_kernel,
        out_shape=jax.ShapeDtypeStruct(below.shape, F32),
        in_specs=[SM, VM, VM, VM],
        out_specs=VM,
        scratch_shapes=sweep_scratch(own, vectors),
        cost_estimate=cost(8 * own.size, 8 * own.size),
    )(offsets, vectors, own, below)


def sweep(place, own, above, below, vectors, offsets, pieces, cut):
    shapes = [jax.ShapeDtypeStruct(own.shape, F32)]
    if cut:
        shapes.append(jax.ShapeDtypeStruct((pieces, own.shape[0], cut), BF16))
    return pl.pallas_call(
        functools.partial(sweep_kernel, cut=cut),
        out_shape=shapes,
        in_specs=[SM, SM, VM, VM, VM, VM],
        out_specs=[VM] * len(shapes),
        scratch_shapes=sweep_scratch(own, vectors),
        cost_estimate=cost(8 * own.size, 8 * own.size),
    )(place, offsets, vectors, own, above, below)


def sweeps(eigen, vectors, offsets, pieces, cut):
    band = vectors.shape[3]
    count, spans = offsets.shape
    assert eigen.shape[1] > (spans + 1) * band
    place = lax.axis_index("row").astype(jnp.int32)[None]
    for at in range(count):
        below = from_behind(eigen[:, :band], "row", -1)
        above = from_behind(overhang(eigen, below, vectors[at], offsets[at]), "row", 1)
        last = at == count - 1
        got = sweep(
            place, eigen, above, below, vectors[at], offsets[at], pieces, cut if last else 0
        )
        eigen = got[0]
    return got


def products_kernel(gathered_ref, eigen_ref, ordered_ref, sums_ref, total_ref, *, dims):
    z_size, x_size, panels, own = dims
    step = pl.program_id(0)
    for z in range(z_size):
        for x in range(x_size):
            for p in range(panels):
                to = ((p * x_size + x) * z_size + z) * own
                at = ((z * x_size + x) * panels + p) * own
                ordered_ref[to : to + own, :] = gathered_ref[at : at + own, :]

    @pl.when(step == 0)
    def _():
        total_ref[...] = jnp.zeros_like(total_ref)

    order = ordered_ref.shape[0]
    reflect = ordered_ref[...]
    total_ref[:, 0:order] += lax.dot_general(
        reflect, reflect, CONTRACT_LAST, preferred_element_type=F32
    )
    total_ref[:, order:] += lax.dot_general(
        reflect, eigen_ref[...], CONTRACT_LAST, preferred_element_type=F32
    )

    @pl.when(step == pl.num_programs(0) - 1)
    def _():
        sums_ref[...] = total_ref[...].astype(BF16)


def block_of(columns):
    tiles = columns // LANE
    return LANE * max(d for d in range(1, 9) if tiles % d == 0)


def products(gathered, eigen, dims):
    order, columns = gathered.shape
    count = eigen.shape[0]
    block = block_of(columns)
    return pl.pallas_call(
        functools.partial(products_kernel, dims=dims),
        grid=(columns // block,),
        in_specs=[
            pl.BlockSpec((order, block), lambda k: (0, k)),
            pl.BlockSpec((count, block), lambda k: (0, k)),
        ],
        out_specs=[
            pl.BlockSpec((order, block), lambda k: (0, k)),
            pl.BlockSpec((order, order + count), lambda k: (0, 0)),
        ],
        out_shape=[
            jax.ShapeDtypeStruct((order, columns), BF16),
            jax.ShapeDtypeStruct((order, order + count), BF16),
        ],
        scratch_shapes=[pltpu.VMEM((order, order + count), F32)],
        compiler_params=pltpu.CompilerParams(dimension_semantics=("arbitrary",)),
        cost_estimate=cost(2 * order * (order + count) * columns, 6 * order * columns),
    )(gathered, eigen)


def small_inverses(grams):
    order = grams[0].shape[0]
    row = lax.broadcasted_iota(jnp.int32, (order, order), 0)
    col = lax.broadcasted_iota(jnp.int32, (order, order), 1)
    eye = row == col
    found = [jnp.where(eye, 2.0 / jnp.where(eye, gram, 1.0), 0.0) for gram in grams]
    size = 1
    while size < order:
        pick = (row // (2 * size) == col // (2 * size)) & (row // size < col // size)
        for at, gram in enumerate(grams):
            part = jnp.where(pick, gram, 0.0)
            if size == 1:
                left = jnp.sum(found[at], axis=1, keepdims=True)
                right = jnp.sum(found[at], axis=0, keepdims=True)
                step = left * part * right
            else:
                step = jnp.dot(part, found[at], precision=HIGH, preferred_element_type=F32)
                step = jnp.dot(found[at], step, precision=HIGH, preferred_element_type=F32)
            found[at] = found[at] - step
        size *= 2
    return found


def correction_kernel(sums_ref, ordered_ref, out_ref, coeffs_ref, *, panels):
    order = ordered_ref.shape[0]
    pieces, count, _ = out_ref.shape

    @pl.when(pl.program_id(0) == 0)
    def _():
        width = order // panels
        parts = width // LANE
        gram = lambda i, j: sums_ref[i : i + LANE, j : j + LANE].astype(F32)
        starts = [k * LANE for k in range(order // LANE)]
        inverses = small_inverses([gram(i, i) for i in starts])
        solved = {}
        for panel in range(panels):
            for part in range(parts - 1, -1, -1):
                i = panel * width + part * LANE
                value = sums_ref[i : i + LANE, order:].astype(F32)
                for j in solved:
                    if j < panel * width:
                        value = value - jnp.dot(
                            sums_ref[i : i + LANE, j : j + LANE],
                            solved[j].astype(BF16),
                            preferred_element_type=F32,
                        )
                    else:
                        value = value - jnp.dot(
                            gram(i, j), solved[j], precision=HIGH, preferred_element_type=F32
                        )
                value = jnp.dot(
                    inverses[i // LANE], value, precision=HIGH, preferred_element_type=F32
                )
                solved[i] = value
        for i in solved:
            coeffs_ref[:, i : i + LANE] = solved[i].T.astype(BF16)

    product = jnp.dot(coeffs_ref[...], ordered_ref[...], preferred_element_type=F32).astype(BF16)
    for at in range(pieces):
        out_ref[at] = product[at * count : (at + 1) * count]


def correction(sums, ordered, pieces, panels):
    order, columns = ordered.shape
    count = sums.shape[1] - order
    block = block_of(columns)
    return pl.pallas_call(
        functools.partial(correction_kernel, panels=panels),
        grid=(columns // block,),
        in_specs=[
            pl.BlockSpec((order, order + count), lambda k: (0, 0)),
            pl.BlockSpec((order, block), lambda k: (0, k)),
        ],
        out_specs=pl.BlockSpec((pieces, count // pieces, block), lambda k: (0, 0, k)),
        out_shape=jax.ShapeDtypeStruct((pieces, count // pieces, columns), BF16),
        scratch_shapes=[pltpu.VMEM((count, order), BF16)],
        compiler_params=pltpu.CompilerParams(dimension_semantics=("arbitrary",)),
        cost_estimate=cost(2 * order * count * columns, 2 * order * columns),
    )(sums, ordered)


def subtract_kernel(eigen_ref, piece_ref, out_ref):
    out_ref[...] = eigen_ref[...] - piece_ref[0].astype(F32)


def subtract(eigen, pieces):
    count, rows, cut = pieces.shape
    return pl.pallas_call(
        subtract_kernel,
        grid=(count,),
        in_specs=[
            pl.BlockSpec((rows, cut), lambda k: (0, k)),
            pl.BlockSpec((1, rows, cut), lambda k: (k, 0, 0)),
        ],
        out_specs=pl.BlockSpec((rows, cut), lambda k: (0, k)),
        out_shape=jax.ShapeDtypeStruct(eigen.shape, F32),
        compiler_params=pltpu.CompilerParams(dimension_semantics=("arbitrary",)),
        cost_estimate=cost(eigen.size, 10 * eigen.size),
    )(eigen, pieces)


def exchange(pieces, axes):
    return lax.all_to_all(pieces, axes, 0, 0, tiled=True)


def local(eigvecs, span_vectors, span_offsets, panels):
    x_size, z_size = lax.axis_size("x"), lax.axis_size("z")
    peers = lax.axis_size("row") * x_size
    count, own, columns = panels.shape
    order = count * own * x_size * z_size
    cut = -(-columns // (LANE * x_size)) * LANE
    padded = jnp.pad(panels, ((0, 0), (0, 0), (0, x_size * cut - columns)))
    pieces = padded.reshape(count, own, x_size, cut).transpose(2, 0, 1, 3)
    mine = exchange(pieces.reshape(x_size, count * own, cut), "x")
    gathered = lax.all_gather(mine.reshape(-1, cut), "z", axis=0, tiled=True)
    eigen, rounded = sweeps(eigvecs, span_vectors, span_offsets, x_size, cut)
    others = exchange(rounded, "x").reshape(-1, cut)
    ordered, sums = products(gathered, others, (z_size, x_size, count, own))
    parts = exchange(sums.reshape(peers, order // peers, -1), ("row", "x"))
    total = jnp.sum(parts.astype(F32), axis=0).astype(BF16)
    sums = exchange(jnp.broadcast_to(total[None], (peers, *total.shape)), ("row", "x"))
    corrections = correction(sums.reshape(order, -1), ordered, x_size, count)
    return subtract(eigen, exchange(corrections, "x"))


def solution(mesh):
    finer = Mesh(mesh.devices.reshape(mesh.shape["row"], 4, 8), ("row", "x", "z"))
    placed = (P(COL, "row"), P(None, "row", None, None), P(None, "row"), P(None, COL, "row"))
    return jax.shard_map(
        local, mesh=finer, in_specs=placed, out_specs=P(COL, "row"), check_vma=False
    )
```

```python
import functools

import jax
import jax.numpy as jnp
from jax import lax
from jax.experimental import pallas as pl
from jax.experimental.pallas import tpu as pltpu
from jax.sharding import Mesh
from jax.sharding import PartitionSpec as P


COL = ("x", "z")
X_SIZE, Z_SIZE = 4, 8
LANE = 128
UNIT = 8
F32 = jnp.float32
BF16 = jnp.bfloat16
CONTRACT_LAST = (((1,), (1,)), ((), ()))
VM = pl.BlockSpec(memory_space=pltpu.VMEM)
SM = pl.BlockSpec(memory_space=pltpu.SMEM)
ANY = pl.BlockSpec(memory_space=pl.ANY)
PEERS = (1, 3, 2)


def call(kernel, out_shape, in_specs, args, scratch=(), flops=0, size=0, vmem=0, outs=None):
    outs = outs or jax.tree.map(lambda _: VM, out_shape)
    return pl.pallas_call(
        kernel,
        out_shape=out_shape,
        in_specs=in_specs,
        out_specs=outs,
        scratch_shapes=list(scratch),
        compiler_params=pltpu.CompilerParams(vmem_limit_bytes=vmem << 20) if vmem else None,
        cost_estimate=pl.CostEstimate(flops=flops, bytes_accessed=size, transcendentals=0),
    )(*args)


def shifted(value, axis, steps):
    count = lax.axis_size(axis)
    return lax.ppermute(value, axis, [(at, (at + steps) % count) for at in range(count)])


def from_behind(value, axis, steps):
    count = lax.axis_size(axis)
    first, last = (max(0, -steps), min(count, count - steps))
    return lax.ppermute(value, axis, [(source, source + steps) for source in range(first, last)])


def span_factors(vectors):
    solved = []
    for i in range(len(vectors)):
        value = vectors[i]
        for j in range(i):
            value = value - jnp.sum(vectors[j] * vectors[i], axis=1, keepdims=True) * solved[j]
        pivot = 0.5 * jnp.sum(vectors[i] * vectors[i], axis=1, keepdims=True)
        solved.append(value / pivot)
    return solved


def lay_pairs(vectors, pairs_ref):
    refl, (spans, band) = len(vectors), vectors[0].shape
    factors = span_factors(vectors)
    for i in range(refl):
        pairs_ref[:, i, 0:band] = vectors[i]
        pairs_ref[:, refl + i, 0:band] = factors[i]
        pairs_ref[:, i, band:] = jnp.zeros((spans, band), F32)
        pairs_ref[:, refl + i, band:] = jnp.zeros((spans, band), F32)


def apply_span(begin, pair, state_ref):
    refl = pair.shape[0] // 2
    base = pl.multiple_of(begin // LANE * LANE, LANE)
    moved = pltpu.roll(pair, begin - base, 1)
    window = state_ref[:, pl.ds(base, pair.shape[1])]
    update = window
    for i in range(refl):
        inner = jnp.sum(window * moved[i : i + 1, :], axis=1, keepdims=True)
        update = update - inner * moved[refl + i : refl + i + 1, :]
    state_ref[:, pl.ds(base, pair.shape[1])] = update


def halo_kernel(offsets_ref, vectors_ref, eigen_ref, down_ref, up_ref, sems):
    sweeps, spans, refl, band = vectors_ref.shape
    rows, columns = eigen_ref.shape
    copies = []
    for at, (ref, begin, count) in enumerate(((down_ref, None, sweeps), (up_ref, 0, sweeps - 1))):
        width = ref.shape[1] - count * band - LANE
        begin = columns - width if begin is None else begin
        copies.append(
            pltpu.make_async_copy(
                eigen_ref.at[:, begin : begin + width], ref.at[:, 0:width], sems.at[at]
            )
        )
        copies[-1].start()
        for sweep in range(count):
            for i in range(refl):
                ref[i * spans : (i + 1) * spans, width + sweep * band : width + (sweep + 1) * band] = (
                    vectors_ref[sweep, :, i, :]
                )
        ref[:, width + count * band :] = jnp.zeros((rows, LANE), F32)
        ref[0:sweeps, width + count * band : width + count * band + spans] = offsets_ref[...].astype(F32)
    for copy in copies:
        copy.wait()


def sweep_kernel(
    place_ref, offsets_ref, upper_offsets_ref, lower_offsets_ref,
    vectors_ref, own_ref, upper_ref, lower_ref,
    out_ref, mine_ref, next_ref, last_ref, far_ref,
    state_ref, pairs_ref, rounded_ref,
):
    sweeps, spans, refl, band = vectors_ref.shape
    rows, columns = own_ref.shape
    left = upper_ref.shape[1] - sweeps * band - LANE
    right = lower_ref.shape[1] - (sweeps - 1) * band - LANE
    state_ref[:, 0:left] = upper_ref[:, 0:left]
    state_ref[:, left : left + columns] = own_ref[...]
    state_ref[:, left + columns :] = lower_ref[:, 0:right]
    first = place_ref[0] == 0
    final = place_ref[0] == place_ref[1] - 1

    def beside(ref, width, sweep, i):
        return ref[i * spans : (i + 1) * spans, width + sweep * band : width + (sweep + 1) * band]

    for sweep in range(sweeps):
        lay_pairs([beside(upper_ref, left, sweep, i) for i in range(refl)], pairs_ref.at[sweep * 3])
        lay_pairs([vectors_ref[sweep, :, i, :] for i in range(refl)], pairs_ref.at[sweep * 3 + 1])
        if sweep < sweeps - 1:
            lay_pairs([beside(lower_ref, right, sweep, i) for i in range(refl)], pairs_ref.at[sweep * 3 + 2])
    for sweep in range(sweeps):

        def from_upper(at, carry, sweep=sweep):
            begin = upper_offsets_ref[sweep, at] - (columns - left)

            @pl.when(jnp.logical_and(begin >= 0, jnp.logical_not(first)))
            def _():
                apply_span(begin, pairs_ref[sweep * 3, at], state_ref)

            return carry

        def from_lower(at, carry, sweep=sweep):
            begin = lower_offsets_ref[sweep, at]

            @pl.when(jnp.logical_and(begin <= right - band, jnp.logical_not(final)))
            def _():
                apply_span(left + columns + begin, pairs_ref[sweep * 3 + 2, at], state_ref)

            return carry

        lax.fori_loop(0, spans, from_upper, 0)
        for at in range(spans):
            apply_span(left + offsets_ref[sweep, at], pairs_ref[sweep * 3 + 1, at], state_ref)
        if sweep < sweeps - 1:
            lax.fori_loop(0, spans, from_lower, 0)
    out_ref[...] = state_ref[:, left : left + columns]
    padded = rounded_ref.shape[1]
    rounded_ref[:, 0:columns] = state_ref[:, left : left + columns].astype(BF16)
    rounded_ref[:, columns:] = jnp.zeros((rows, padded - columns), BF16)
    cut = mine_ref.shape[1]
    for step, ref in ((0, mine_ref), (PEERS[0], next_ref), (PEERS[1], last_ref), (PEERS[2], far_ref)):
        at = pl.multiple_of((place_ref[2] + step) % X_SIZE * cut, LANE)
        ref[...] = rounded_ref[:, pl.ds(at, cut)]


def sweep_all(place, eigen, vectors, offsets, cut):
    sweeps, spans, refl, band = vectors.shape
    rows, columns = eigen.shape
    left, right = sweeps * spans * band, ((sweeps - 1) * spans + 1) * band
    assert left + right + band < columns and spans * refl == rows
    wide = lambda width: jax.ShapeDtypeStruct((rows, width), F32)
    down, up = call(
        halo_kernel,
        [wide(left + sweeps * band + LANE), wide(right + (sweeps - 1) * band + LANE)],
        [VM, VM, ANY],
        (offsets, vectors, eigen),
        [pltpu.SemaphoreType.DMA((2,))],
        flops=eigen.size,
        size=4 * eigen.size,
        vmem=8,
    )
    upper = from_behind(down, "row", 1)
    lower = from_behind(up, "row", -1)
    upper_offsets = upper[0:sweeps, -LANE : spans - LANE].astype(jnp.int32)
    lower_offsets = lower[0:sweeps, -LANE : spans - LANE].astype(jnp.int32)
    return call(
        sweep_kernel,
        [jax.ShapeDtypeStruct(eigen.shape, F32)]
        + [jax.ShapeDtypeStruct((rows, cut), BF16)] * 4,
        [SM] * 4 + [VM] * 4,
        (place, offsets, upper_offsets, lower_offsets, vectors, eigen, upper, lower),
        [
            pltpu.VMEM((rows, left + columns + right), F32),
            pltpu.VMEM((3 * sweeps, spans, 2 * refl, 2 * band), F32),
            pltpu.VMEM((rows, X_SIZE * cut), BF16),
        ],
        flops=40 * eigen.size,
        size=12 * eigen.size,
        vmem=14,
    )


def pack_kernel(place_ref, panels_ref, *refs):
    wide_ref = refs[-1]
    panels, own, columns = panels_ref.shape
    for p in range(panels):
        wide_ref[p * own : (p + 1) * own, 0:columns] = panels_ref[p]
    wide_ref[:, columns:] = jnp.zeros((panels * own, wide_ref.shape[1] - columns), BF16)
    for step, ref in zip((0, *PEERS), refs):
        cut = ref.shape[1]
        at = pl.multiple_of((place_ref[2] + step) % X_SIZE * cut, LANE)
        ref[...] = wide_ref[:, pl.ds(at, cut)]


def pack(place, panels, cut):
    rows = panels.shape[0] * panels.shape[1]
    return call(
        pack_kernel,
        [jax.ShapeDtypeStruct((rows, cut), BF16)] * 4,
        [SM, VM],
        (place, panels),
        [pltpu.VMEM((rows, X_SIZE * cut), BF16)],
        flops=panels.size,
        size=4 * panels.size,
        vmem=4,
    )


def piece_shapes(rows, cut):
    full, half = jax.ShapeDtypeStruct((rows, cut), BF16), jax.ShapeDtypeStruct((rows // 2, cut), BF16)
    return [full, full, full, half, half]


def traded(pieces):
    steps = (1, -1, 2) if len(pieces) == 4 else (1, -1, 2, -2)
    got = []
    for piece, step in zip(pieces[1:], steps):
        got.append(shifted(piece, "x", step))
    return got


def ring(block, far):
    ahead = behind = block
    found = [(0, block)]
    for step in range(1, Z_SIZE // 2):
        ahead = shifted(ahead, "z", 1)
        behind = shifted(behind, "z", -1)
        found += [(step, ahead), (Z_SIZE - step, behind)]
    found.append((Z_SIZE // 2, shifted(ahead if far > 0 else behind, "z", far)))
    return found


def products_kernel(place_ref, *refs, spots, own, rows):
    blocks, (mine, one, two, far) = refs[: len(spots)], refs[len(spots) : len(spots) + 4]
    ordered_ref, sums_ref, eigen_ref = refs[len(spots) + 4 :]
    order = ordered_ref.shape[0]
    x, z = place_ref[2], place_ref[3]
    for ref, units in zip(blocks, spots):
        for at, (back_z, back_x, panel) in enumerate(units):
            source = (x + X_SIZE - back_x) % X_SIZE * Z_SIZE + (z + Z_SIZE - back_z) % Z_SIZE
            to = pl.multiple_of(panel * (order // 2) + source * own, UNIT)
            ordered_ref[pl.ds(to, own), :] = ref[at * own : (at + 1) * own, :]
    for back, ref in ((0, mine), (1, one), (3, two), (2, far)):
        to = pl.multiple_of((x + X_SIZE - back) % X_SIZE * rows, UNIT)
        eigen_ref[pl.ds(to, ref.shape[0]), :] = ref[...]

    def put(value, at):
        sums_ref[at * LANE : (at + 1) * LANE] = value.astype(BF16)

    def dot(first, count, other):
        return lax.dot_general(
            ordered_ref[first : first + count, :], other, CONTRACT_LAST, preferred_element_type=F32
        )

    width = order // 2
    early = dot(0, order, ordered_ref[0:width, :])
    late = dot(width, width, ordered_ref[width:, :])
    inner = dot(0, order, eigen_ref[...])
    tile = lambda value, i, j: value[i * LANE : (i + 1) * LANE, j * LANE : (j + 1) * LANE]
    for i in range(4):
        put(tile(inner, i, 0), i)
    for at, (i, j) in enumerate(((0, 0), (0, 1), (1, 1), (2, 0), (2, 1), (3, 0), (3, 1))):
        put(tile(early, i, j), 4 + at)
    for at, (i, j) in enumerate(((0, 0), (0, 1), (1, 1))):
        put(tile(late, i, j), 11 + at)


TILES = {
    at: 4 + k
    for k, at in enumerate(
        ((0, 0), (0, 1), (1, 1), (2, 0), (2, 1), (3, 0), (3, 1), (2, 2), (2, 3), (3, 3))
    )
}


def products(place, found, pieces, spots, own, order, rows):
    cut = pieces[0].shape[1]
    return call(
        functools.partial(products_kernel, spots=spots, own=own, rows=rows),
        [
            jax.ShapeDtypeStruct((order, cut), BF16),
            jax.ShapeDtypeStruct(((4 + len(TILES)) * LANE, LANE), BF16),
        ],
        [SM] + [VM] * (len(found) + len(pieces)),
        (place, *found, *pieces),
        [pltpu.VMEM((LANE, cut), BF16)],
        flops=2 * order * (order + LANE) * cut,
        size=6 * order * cut,
        vmem=18,
    )


def split(value):
    high = value.astype(BF16)
    return high, (value - high.astype(F32)).astype(BF16)


def fine_dot(a, b):
    a0, a1 = a if isinstance(a, tuple) else split(a)
    b0, b1 = b if isinstance(b, tuple) else split(b)
    dot = functools.partial(jnp.dot, preferred_element_type=F32)
    total = dot(a0, b0)
    if b1 is not None:
        total = total + dot(a0, b1)
    if a1 is not None:
        total = total + dot(a1, b0)
    return total


def small_inverses(grams):
    order = grams[0].shape[0]
    row = lax.broadcasted_iota(jnp.int32, (order, order), 0)
    col = lax.broadcasted_iota(jnp.int32, (order, order), 1)
    eye = row == col
    wide = [gram.astype(F32) for gram in grams]
    found = [jnp.where(eye, 2.0 / jnp.where(eye, gram, 1.0), 0.0) for gram in wide]
    size = 1
    while size < order:
        pick = (row // (2 * size) == col // (2 * size)) & (row // size < col // size)
        parts = [jnp.where(pick, gram, 0.0) for gram in wide]
        if size == 1:
            steps = [
                jnp.sum(f, axis=1, keepdims=True) * part * jnp.sum(f, axis=0, keepdims=True)
                for f, part in zip(found, parts)
            ]
        else:
            halves = [split(f) for f in found]
            steps = [fine_dot((part.astype(BF16), None), f) for part, f in zip(parts, halves)]
            steps = [fine_dot(f, step) for f, step in zip(halves, steps)]
        found = [f - step for f, step in zip(found, steps)]
        size *= 2
    return found


def correction_kernel(
    place_ref, sums_ref, ordered_ref, mine_ref, next_ref, last_ref, one_ref, two_ref, coeffs_ref
):
    tile = lambda at: sums_ref[at * LANE : (at + 1) * LANE, :]
    gram = lambda i, j: tile(TILES[i, j])
    inverses = [split(f) for f in small_inverses([gram(i, i) for i in range(4)])]
    solved = {}
    for i in (1, 0, 3, 2):
        value = tile(i).astype(F32)
        for j in solved:
            if j // 2 < i // 2:
                known = (solved[j].astype(BF16), None)
            else:
                known = solved[j]
            value = value - fine_dot((gram(i, j), None), known)
        solved[i] = fine_dot(inverses[i], value)
        coeffs_ref[:, i * LANE : (i + 1) * LANE] = solved[i].T.astype(BF16)
    rows = mine_ref.shape[0]
    x = place_ref[2]

    def product(step, shift, count):
        at = pl.multiple_of((x + step) % X_SIZE * rows + shift, UNIT)
        return jnp.dot(
            coeffs_ref[pl.ds(at, count), :], ordered_ref[...], preferred_element_type=F32
        )

    next_ref[...] = product(PEERS[0], 0, rows).astype(BF16)
    last_ref[...] = product(PEERS[1], 0, rows).astype(BF16)
    far = product(PEERS[2], 0, rows).astype(BF16)
    one_ref[...] = far[0 : rows // 2]
    two_ref[...] = far[rows // 2 :]
    mine_ref[...] = product(0, 0, rows).astype(BF16)


def correction(place, sums, ordered, rows):
    order, cut = ordered.shape
    return call(
        correction_kernel,
        piece_shapes(rows, cut),
        [SM, VM, VM],
        (place, sums, ordered),
        [pltpu.VMEM((LANE, order), BF16)],
        flops=2 * order * LANE * cut,
        size=4 * order * cut,
        vmem=24,
    )


def subtract_kernel(place_ref, eigen_ref, mine, one, two, half0, half1, out_ref):
    rows, columns = eigen_ref.shape
    cut = mine.shape[1]
    half = rows // 2
    sources = {0: ((0, mine),), 1: ((0, one),), 3: ((0, two),), 2: ((0, half0), (half, half1))}
    for at in range(X_SIZE):
        begin, span = at * cut, min(cut, columns - at * cut)
        for back, refs in sources.items():

            @pl.when((place_ref[2] + X_SIZE - back) % X_SIZE == at)
            def _(refs=refs, begin=begin, span=span):
                for row, ref in refs:
                    high = row + ref.shape[0]
                    out_ref[row:high, begin : begin + span] = (
                        eigen_ref[row:high, begin : begin + span] - ref[:, 0:span].astype(F32)
                    )


def subtract(place, eigen, pieces):
    return call(
        subtract_kernel,
        jax.ShapeDtypeStruct(eigen.shape, F32),
        [SM] + [VM] * 6,
        (place, eigen, *pieces),
        flops=eigen.size,
        size=10 * eigen.size,
        vmem=10,
    )


def total_kernel(parts_ref, out_ref):
    total = parts_ref[0].astype(F32)
    for at in range(1, parts_ref.shape[0]):
        total = total + parts_ref[at].astype(F32)
    total = total.astype(BF16)
    for at in range(parts_ref.shape[0]):
        out_ref[at] = total


def total_for_all(parts):
    return call(
        total_kernel,
        jax.ShapeDtypeStruct(parts.shape, BF16),
        [VM],
        (parts,),
        flops=parts.size,
        size=4 * parts.size,
        vmem=4,
    )


def exchange(pieces, axes):
    return lax.all_to_all(pieces, axes, 0, 0, tiled=True)


def inner(eigvecs, span_vectors, span_offsets, panels):
    assert (lax.axis_size("x"), lax.axis_size("z")) == (X_SIZE, Z_SIZE)
    peers = lax.axis_size("row") * X_SIZE
    count, own, columns = panels.shape
    rows = eigvecs.shape[0]
    order = count * own * X_SIZE * Z_SIZE
    cut = -(-columns // (LANE * X_SIZE)) * LANE
    place = jnp.stack(
        [lax.axis_index("row"), lax.axis_size("row"), lax.axis_index("x"), lax.axis_index("z")]
    ).astype(jnp.int32)

    packed = pack(place, panels, cut)
    swept = sweep_all(place, eigvecs, span_vectors, span_offsets, cut)
    eigen, pieces = swept[0], swept[1:]
    one, two, far = traded(packed)
    found, spots = [], []
    for at, (pair, sources) in enumerate((((packed[0], one), (0, 1)), ((two, far), (3, 2)))):
        unit = [(back_x, panel) for back_x in sources for panel in range(count)]
        for back, block in ring(jnp.concatenate(pair, axis=0), 1 - 2 * at):
            found.append(block)
            spots.append([(back, back_x, panel) for back_x, panel in unit])
    others = [pieces[0], *traded(pieces)]
    ordered, sums = products(place, found, others, spots, own, order, rows)

    parts = exchange(sums.reshape(peers, -1, LANE), ("row", "x"))
    sums = exchange(total_for_all(parts), ("row", "x"))
    corrections = correction(place, sums.reshape(-1, LANE), ordered, rows)
    return subtract(place, eigen, [corrections[0], *traded(corrections)])


def solution(mesh):
    finer = Mesh(
        mesh.devices.reshape(mesh.shape["row"], X_SIZE, Z_SIZE), ("row", "x", "z")
    )
    placed = (P(COL, "row"), P(None, "row", None, None), P(None, "row"), P(None, COL, "row"))
    return jax.shard_map(
        inner, mesh=finer, in_specs=placed, out_specs=P(COL, "row"), check_vma=False
    )
```

```python
import functools

import jax
import jax.numpy as jnp
from jax import lax
from jax.experimental import pallas as pl
from jax.experimental.pallas import tpu as pltpu
from jax.sharding import Mesh
from jax.sharding import PartitionSpec as P


COL = ("x", "z")
X_SIZE, Z_SIZE = 4, 8
LANE = 128
FRONT_MB = 60
UNIT = 8
F32 = jnp.float32
BF16 = jnp.bfloat16
CONTRACT_LAST = (((1,), (1,)), ((), ()))
VM = pl.BlockSpec(memory_space=pltpu.VMEM)
SM = pl.BlockSpec(memory_space=pltpu.SMEM)
ANY = pl.BlockSpec(memory_space=pl.ANY)
PEERS = (1, 3, 2)


def call(kernel, out_shape, in_specs, args, scratch=(), flops=0, size=0, vmem=0, outs=None):
    outs = outs or jax.tree.map(lambda _: VM, out_shape)
    return pl.pallas_call(
        kernel,
        out_shape=out_shape,
        in_specs=in_specs,
        out_specs=outs,
        scratch_shapes=list(scratch),
        compiler_params=pltpu.CompilerParams(vmem_limit_bytes=vmem << 20) if vmem else None,
        cost_estimate=pl.CostEstimate(flops=flops, bytes_accessed=size, transcendentals=0),
    )(*args)


def shifted(value, axis, steps):
    count = lax.axis_size(axis)
    return lax.ppermute(value, axis, [(at, (at + steps) % count) for at in range(count)])


def from_behind(value, axis, steps):
    count = lax.axis_size(axis)
    first, last = (max(0, -steps), min(count, count - steps))
    return lax.ppermute(value, axis, [(source, source + steps) for source in range(first, last)])


def span_factors(vectors):
    solved = []
    for i in range(len(vectors)):
        value = vectors[i]
        for j in range(i):
            value = value - jnp.sum(vectors[j] * vectors[i], axis=1, keepdims=True) * solved[j]
        pivot = 0.5 * jnp.sum(vectors[i] * vectors[i], axis=1, keepdims=True)
        solved.append(value / pivot)
    return solved


def lay_pairs(vectors, pairs_ref):
    refl, (spans, band) = len(vectors), vectors[0].shape
    factors = span_factors(vectors)
    for i in range(refl):
        pairs_ref[:, i, 0:band] = vectors[i]
        pairs_ref[:, refl + i, 0:band] = factors[i]
        pairs_ref[:, i, band:] = jnp.zeros((spans, band), F32)
        pairs_ref[:, refl + i, band:] = jnp.zeros((spans, band), F32)


def apply_span(begin, pair, state_ref):
    refl = pair.shape[0] // 2
    base = pl.multiple_of(begin // LANE * LANE, LANE)
    moved = pltpu.roll(pair, begin - base, 1)
    window = state_ref[:, pl.ds(base, pair.shape[1])]
    update = window
    for i in range(refl):
        inner = jnp.sum(window * moved[i : i + 1, :], axis=1, keepdims=True)
        update = update - inner * moved[refl + i : refl + i + 1, :]
    state_ref[:, pl.ds(base, pair.shape[1])] = update


def front_kernel(
    offsets_ref, vectors_ref, panels_ref, eigen_ref, *refs
):
    down_ref, up_ref, wide_ref, sems = refs[-4:]
    sweeps, spans, refl, band = vectors_ref.shape
    rows, columns = eigen_ref.shape
    panels, own, _ = panels_ref.shape
    moves = [
        pltpu.make_async_copy(
            panels_ref.at[p], wide_ref.at[p * own : (p + 1) * own, 0:columns], sems.at[p]
        )
        for p in range(panels)
    ]
    halos = ((down_ref, None, sweeps), (up_ref, 0, sweeps - 1))
    for ref, begin, count in halos:
        width = ref.shape[1] - count * band - LANE
        begin = columns - width if begin is None else begin
        moves.append(
            pltpu.make_async_copy(
                eigen_ref.at[:, begin : begin + width], ref.at[:, 0:width], sems.at[len(moves)]
            )
        )
    for move in moves:
        move.start()
    wide_ref[:, columns:] = jnp.zeros((panels * own, wide_ref.shape[1] - columns), BF16)
    for ref, _, count in halos:
        width = ref.shape[1] - count * band - LANE
        for sweep in range(count):
            for i in range(refl):
                ref[i * spans : (i + 1) * spans, width + sweep * band : width + (sweep + 1) * band] = (
                    vectors_ref[sweep, :, i, :]
                )
        ref[:, width + count * band :] = jnp.zeros((rows, LANE), F32)
        ref[0:sweeps, width + count * band : width + count * band + spans] = offsets_ref[...].astype(F32)
    for move in moves[:panels]:
        move.wait()
    for step, ref in zip((0, *PEERS), refs):
        cut = ref.shape[1]
        at = pl.multiple_of((lax.axis_index("x") + step) % X_SIZE * cut, LANE)
        ref[...] = wide_ref[:, pl.ds(at, cut)]
    for move in moves[panels:]:
        move.wait()


def halo_sizes(vectors):
    sweeps, spans, _, band = vectors.shape
    return sweeps * spans * band, ((sweeps - 1) * spans + 1) * band


def front(eigen, vectors, offsets, panels, cut):
    sweeps, _, _, band = vectors.shape
    rows = eigen.shape[0]
    left, right = halo_sizes(vectors)
    wide = lambda width: jax.ShapeDtypeStruct((rows, width), F32)
    high = panels.shape[0] * panels.shape[1]
    return call(
        front_kernel,
        [jax.ShapeDtypeStruct((high, cut), BF16)] * 4
        + [wide(left + sweeps * band + LANE), wide(right + (sweeps - 1) * band + LANE)],
        [VM, VM, ANY, ANY],
        (offsets, vectors, panels, eigen),
        [pltpu.VMEM((high, X_SIZE * cut), BF16), pltpu.SemaphoreType.DMA((panels.shape[0] + 2,))],
        flops=panels.size,
        size=4 * panels.size,
        vmem=FRONT_MB,
    )


def sweep_kernel(
    offsets_ref, upper_offsets_ref, lower_offsets_ref,
    vectors_ref, own_ref, upper_ref, lower_ref,
    out_ref, mine_ref, next_ref, last_ref, far_ref,
    state_ref, pairs_ref, rounded_ref,
):
    sweeps, spans, refl, band = vectors_ref.shape
    rows, columns = own_ref.shape
    left = upper_ref.shape[1] - sweeps * band - LANE
    right = lower_ref.shape[1] - (sweeps - 1) * band - LANE
    state_ref[:, 0:left] = upper_ref[:, 0:left]
    state_ref[:, left : left + columns] = own_ref[...]
    state_ref[:, left + columns :] = lower_ref[:, 0:right]
    first = lax.axis_index("row") == 0
    final = lax.axis_index("row") == lax.axis_size("row") - 1

    def beside(ref, width, sweep, i):
        return ref[i * spans : (i + 1) * spans, width + sweep * band : width + (sweep + 1) * band]

    for sweep in range(sweeps):
        lay_pairs([beside(upper_ref, left, sweep, i) for i in range(refl)], pairs_ref.at[sweep * 3])
        lay_pairs([vectors_ref[sweep, :, i, :] for i in range(refl)], pairs_ref.at[sweep * 3 + 1])
        if sweep < sweeps - 1:
            lay_pairs([beside(lower_ref, right, sweep, i) for i in range(refl)], pairs_ref.at[sweep * 3 + 2])
    for sweep in range(sweeps):

        def from_upper(at, carry, sweep=sweep):
            begin = upper_offsets_ref[sweep, at] - (columns - left)

            @pl.when(jnp.logical_and(begin >= 0, jnp.logical_not(first)))
            def _():
                apply_span(begin, pairs_ref[sweep * 3, at], state_ref)

            return carry

        def from_lower(at, carry, sweep=sweep):
            begin = lower_offsets_ref[sweep, at]

            @pl.when(jnp.logical_and(begin <= right - band, jnp.logical_not(final)))
            def _():
                apply_span(left + columns + begin, pairs_ref[sweep * 3 + 2, at], state_ref)

            return carry

        lax.fori_loop(0, spans, from_upper, 0)
        for at in range(spans):
            apply_span(left + offsets_ref[sweep, at], pairs_ref[sweep * 3 + 1, at], state_ref)
        if sweep < sweeps - 1:
            lax.fori_loop(0, spans, from_lower, 0)
    out_ref[...] = state_ref[:, left : left + columns]
    padded = rounded_ref.shape[1]
    rounded_ref[:, 0:columns] = state_ref[:, left : left + columns].astype(BF16)
    rounded_ref[:, columns:] = jnp.zeros((rows, padded - columns), BF16)
    cut = mine_ref.shape[1]
    for step, ref in ((0, mine_ref), (PEERS[0], next_ref), (PEERS[1], last_ref), (PEERS[2], far_ref)):
        at = pl.multiple_of((lax.axis_index("x") + step) % X_SIZE * cut, LANE)
        ref[...] = rounded_ref[:, pl.ds(at, cut)]


def sweep_all(eigen, vectors, offsets, down, up, cut):
    sweeps, spans, refl, band = vectors.shape
    rows, columns = eigen.shape
    left, right = halo_sizes(vectors)
    assert left + right + band < columns and spans * refl == rows
    upper = from_behind(down, "row", 1)
    lower = from_behind(up, "row", -1)
    upper_offsets = upper[0:sweeps, -LANE : spans - LANE].astype(jnp.int32)
    lower_offsets = lower[0:sweeps, -LANE : spans - LANE].astype(jnp.int32)
    return call(
        sweep_kernel,
        [jax.ShapeDtypeStruct(eigen.shape, F32)]
        + [jax.ShapeDtypeStruct((rows, cut), BF16)] * 4,
        [SM] * 3 + [VM] * 4,
        (offsets, upper_offsets, lower_offsets, vectors, eigen, upper, lower),
        [
            pltpu.VMEM((rows, left + columns + right), F32),
            pltpu.VMEM((3 * sweeps, spans, 2 * refl, 2 * band), F32),
            pltpu.VMEM((rows, X_SIZE * cut), BF16),
        ],
        flops=40 * eigen.size,
        size=12 * eigen.size,
        vmem=14,
    )


def piece_shapes(rows, cut):
    full, half = jax.ShapeDtypeStruct((rows, cut), BF16), jax.ShapeDtypeStruct((rows // 2, cut), BF16)
    return [full, full, full, half, half]


def traded(pieces):
    steps = (1, -1, 2) if len(pieces) == 4 else (1, -1, 2, -2)
    got = []
    for piece, step in zip(pieces[1:], steps):
        got.append(shifted(piece, "x", step))
    return got


def ring(block, far):
    ahead = behind = block
    found = [(0, block)]
    for step in range(1, Z_SIZE // 2):
        ahead = shifted(ahead, "z", 1)
        behind = shifted(behind, "z", -1)
        found += [(step, ahead), (Z_SIZE - step, behind)]
    found.append((Z_SIZE // 2, shifted(ahead if far > 0 else behind, "z", far)))
    return found


def products_kernel(*refs, spots, own, rows):
    blocks, (mine, one, two, far) = refs[: len(spots)], refs[len(spots) : len(spots) + 4]
    ordered_ref, sums_ref, eigen_ref = refs[len(spots) + 4 :]
    order = ordered_ref.shape[0]
    x, z = lax.axis_index("x"), lax.axis_index("z")
    for ref, units in zip(blocks, spots):
        for at, (back_z, back_x, panel) in enumerate(units):
            source = (x + X_SIZE - back_x) % X_SIZE * Z_SIZE + (z + Z_SIZE - back_z) % Z_SIZE
            to = pl.multiple_of(panel * (order // 2) + source * own, UNIT)
            ordered_ref[pl.ds(to, own), :] = ref[at * own : (at + 1) * own, :]
    for back, ref in ((0, mine), (1, one), (3, two), (2, far)):
        to = pl.multiple_of((x + X_SIZE - back) % X_SIZE * rows, UNIT)
        eigen_ref[pl.ds(to, ref.shape[0]), :] = ref[...]

    def put(value, at):
        sums_ref[at * LANE : (at + 1) * LANE] = value.astype(BF16)

    def dot(first, count, other):
        return lax.dot_general(
            ordered_ref[first : first + count, :], other, CONTRACT_LAST, preferred_element_type=F32
        )

    width = order // 2
    early = dot(0, order, ordered_ref[0:width, :])
    late = dot(width, width, ordered_ref[width:, :])
    inner = dot(0, order, eigen_ref[...])
    tile = lambda value, i, j: value[i * LANE : (i + 1) * LANE, j * LANE : (j + 1) * LANE]
    for i in range(4):
        put(tile(inner, i, 0), i)
    for at, (i, j) in enumerate(((0, 0), (0, 1), (1, 1), (2, 0), (2, 1), (3, 0), (3, 1))):
        put(tile(early, i, j), 4 + at)
    for at, (i, j) in enumerate(((0, 0), (0, 1), (1, 1))):
        put(tile(late, i, j), 11 + at)


TILES = {
    at: 4 + k
    for k, at in enumerate(
        ((0, 0), (0, 1), (1, 1), (2, 0), (2, 1), (3, 0), (3, 1), (2, 2), (2, 3), (3, 3))
    )
}


def products(found, pieces, spots, own, order, rows):
    cut = pieces[0].shape[1]
    return call(
        functools.partial(products_kernel, spots=spots, own=own, rows=rows),
        [
            jax.ShapeDtypeStruct((order, cut), BF16),
            jax.ShapeDtypeStruct(((4 + len(TILES)) * LANE, LANE), BF16),
        ],
        [VM] * (len(found) + len(pieces)),
        (*found, *pieces),
        [pltpu.VMEM((LANE, cut), BF16)],
        flops=2 * order * (order + LANE) * cut,
        size=6 * order * cut,
        vmem=18,
    )


def split(value):
    high = value.astype(BF16)
    return high, (value - high.astype(F32)).astype(BF16)


def fine_dot(a, b):
    a0, a1 = a if isinstance(a, tuple) else split(a)
    b0, b1 = b if isinstance(b, tuple) else split(b)
    dot = functools.partial(jnp.dot, preferred_element_type=F32)
    total = dot(a0, b0)
    if b1 is not None:
        total = total + dot(a0, b1)
    if a1 is not None:
        total = total + dot(a1, b0)
    return total


def small_inverses(grams):
    order = grams[0].shape[0]
    row = lax.broadcasted_iota(jnp.int32, (order, order), 0)
    col = lax.broadcasted_iota(jnp.int32, (order, order), 1)
    eye = row == col
    wide = [gram.astype(F32) for gram in grams]
    found = [jnp.where(eye, 2.0 / jnp.where(eye, gram, 1.0), 0.0) for gram in wide]
    size = 1
    while size < order:
        pick = (row // (2 * size) == col // (2 * size)) & (row // size < col // size)
        parts = [jnp.where(pick, gram, 0.0) for gram in wide]
        if size == 1:
            steps = [
                jnp.sum(f, axis=1, keepdims=True) * part * jnp.sum(f, axis=0, keepdims=True)
                for f, part in zip(found, parts)
            ]
        else:
            halves = [split(f) for f in found]
            steps = [fine_dot((part.astype(BF16), None), f) for part, f in zip(parts, halves)]
            steps = [fine_dot(f, step) for f, step in zip(halves, steps)]
        found = [f - step for f, step in zip(found, steps)]
        size *= 2
    return found


def correction_kernel(
    sums_ref, ordered_ref, mine_ref, next_ref, last_ref, one_ref, two_ref, coeffs_ref
):
    rows = mine_ref.shape[0]
    tile = lambda at: sums_ref[at * LANE : (at + 1) * LANE, :]
    gram = lambda i, j: tile(TILES[i, j])
    inverses = [split(f) for f in small_inverses([gram(i, i) for i in range(4)])]
    solved = {}
    for i in (1, 0, 3, 2):
        value = tile(i).astype(F32)
        for j in solved:
            if j // 2 < i // 2:
                known = (solved[j].astype(BF16), None)
            else:
                known = solved[j]
            value = value - fine_dot((gram(i, j), None), known)
        solved[i] = fine_dot(inverses[i], value)
        turned = solved[i].T.astype(BF16)
        for x in range(X_SIZE):
            to = pl.multiple_of((x + X_SIZE - lax.axis_index("x")) % X_SIZE * rows, UNIT)
            coeffs_ref[pl.ds(to, rows), i * LANE : (i + 1) * LANE] = turned[x * rows : (x + 1) * rows]
    product = jnp.dot(
        coeffs_ref[...], ordered_ref[...], preferred_element_type=F32
    ).astype(BF16)
    piece = lambda step: product[step * rows : (step + 1) * rows]
    mine_ref[...] = piece(0)
    next_ref[...] = piece(PEERS[0])
    last_ref[...] = piece(PEERS[1])
    one_ref[...] = piece(PEERS[2])[0 : rows // 2]
    two_ref[...] = piece(PEERS[2])[rows // 2 :]


def correction(sums, ordered, rows):
    order, cut = ordered.shape
    return call(
        correction_kernel,
        piece_shapes(rows, cut),
        [VM, VM],
        (sums, ordered),
        [pltpu.VMEM((LANE, order), BF16)],
        flops=2 * order * LANE * cut,
        size=4 * order * cut,
        vmem=24,
    )


def subtract_kernel(eigen_ref, mine, one, two, half0, half1, out_ref, held_ref, sems):
    rows, columns = eigen_ref.shape
    cut = mine.shape[1]
    half = rows // 2
    sources = {0: ((0, mine),), 1: ((0, one),), 3: ((0, two),), 2: ((0, half0), (half, half1))}
    leaves = []
    for at in range(X_SIZE):
        begin, span = at * cut, min(cut, columns - at * cut)
        for back, refs in sources.items():

            @pl.when((lax.axis_index("x") + X_SIZE - back) % X_SIZE == at)
            def _(refs=refs, begin=begin, span=span):
                for row, ref in refs:
                    high = row + ref.shape[0]
                    held_ref[row:high, begin : begin + span] = (
                        eigen_ref[row:high, begin : begin + span] - ref[:, 0:span].astype(F32)
                    )

        chunk = slice(begin, begin + span)
        leaves.append(
            pltpu.make_async_copy(held_ref.at[:, chunk], out_ref.at[:, chunk], sems.at[at])
        )
        leaves[-1].start()
    for leave in leaves:
        leave.wait()


def subtract(eigen, pieces):
    return call(
        subtract_kernel,
        jax.ShapeDtypeStruct(eigen.shape, F32),
        [VM] * 6,
        (eigen, *pieces),
        [pltpu.VMEM(eigen.shape, F32), pltpu.SemaphoreType.DMA((X_SIZE,))],
        flops=eigen.size,
        size=10 * eigen.size,
        vmem=12,
        outs=ANY,
    )


def total_kernel(parts_ref, out_ref):
    total = parts_ref[0].astype(F32)
    for at in range(1, parts_ref.shape[0]):
        total = total + parts_ref[at].astype(F32)
    total = total.astype(BF16)
    for at in range(parts_ref.shape[0]):
        out_ref[at] = total


def total_for_all(parts):
    return call(
        total_kernel,
        jax.ShapeDtypeStruct(parts.shape, BF16),
        [VM],
        (parts,),
        flops=parts.size,
        size=4 * parts.size,
        vmem=4,
    )


def exchange(pieces, axes):
    return lax.all_to_all(pieces, axes, 0, 0, tiled=True)


def inner(eigvecs, span_vectors, span_offsets, panels):
    assert (lax.axis_size("x"), lax.axis_size("z")) == (X_SIZE, Z_SIZE)
    peers = lax.axis_size("row") * X_SIZE
    count, own, columns = panels.shape
    rows = eigvecs.shape[0]
    order = count * own * X_SIZE * Z_SIZE
    cut = -(-columns // (LANE * X_SIZE)) * LANE
    *packed, down, up = front(eigvecs, span_vectors, span_offsets, panels, cut)
    swept = sweep_all(eigvecs, span_vectors, span_offsets, down, up, cut)
    eigen, pieces = swept[0], swept[1:]
    one, two, far = traded(packed)
    found, spots = [], []
    for at, (pair, sources) in enumerate((((packed[0], one), (0, 1)), ((two, far), (3, 2)))):
        unit = [(back_x, panel) for back_x in sources for panel in range(count)]
        for back, block in ring(jnp.concatenate(pair, axis=0), 1 - 2 * at):
            found.append(block)
            spots.append([(back, back_x, panel) for back_x, panel in unit])
    others = [pieces[0], *traded(pieces)]
    ordered, sums = products(found, others, spots, own, order, rows)

    parts = exchange(sums.reshape(peers, -1, LANE), ("row", "x"))
    sums = exchange(total_for_all(parts), ("row", "x"))
    corrections = correction(sums.reshape(-1, LANE), ordered, rows)
    return subtract(eigen, [corrections[0], *traded(corrections)])


def solution(mesh):
    finer = Mesh(
        mesh.devices.reshape(mesh.shape["row"], X_SIZE, Z_SIZE), ("row", "x", "z")
    )
    placed = (P(COL, "row"), P(None, "row", None, None), P(None, "row"), P(None, COL, "row"))
    return jax.shard_map(
        inner, mesh=finer, in_specs=placed, out_specs=P(COL, "row"), check_vma=False
    )
```

```python
import functools

import jax
import jax.numpy as jnp
from jax import lax
from jax.experimental import pallas as pl
from jax.experimental.pallas import tpu as pltpu
from jax.sharding import Mesh
from jax.sharding import PartitionSpec as P


COL = ("x", "z")
X_SIZE, Z_SIZE = 4, 8
LANE = 128
GROUP = 4
FRONT_MB = 60
UNIT = 8
F32 = jnp.float32
BF16 = jnp.bfloat16
CONTRACT_LAST = (((1,), (1,)), ((), ()))
VM = pl.BlockSpec(memory_space=pltpu.VMEM)
SM = pl.BlockSpec(memory_space=pltpu.SMEM)
ANY = pl.BlockSpec(memory_space=pl.ANY)
PEERS = (1, 3, 2)


def call(kernel, out_shape, in_specs, args, scratch=(), flops=0, size=0, vmem=0, outs=None):
    outs = outs or jax.tree.map(lambda _: VM, out_shape)
    return pl.pallas_call(
        kernel,
        out_shape=out_shape,
        in_specs=in_specs,
        out_specs=outs,
        scratch_shapes=list(scratch),
        compiler_params=pltpu.CompilerParams(vmem_limit_bytes=vmem << 20) if vmem else None,
        cost_estimate=pl.CostEstimate(flops=flops, bytes_accessed=size, transcendentals=0),
    )(*args)


def shifted(value, axis, steps):
    count = lax.axis_size(axis)
    return lax.ppermute(value, axis, [(at, (at + steps) % count) for at in range(count)])


def from_behind(value, axis, steps):
    count = lax.axis_size(axis)
    first, last = (max(0, -steps), min(count, count - steps))
    return lax.ppermute(value, axis, [(source, source + steps) for source in range(first, last)])


def span_factors(vectors):
    solved = []
    for i in range(len(vectors)):
        value = vectors[i]
        for j in range(i):
            value = value - jnp.sum(vectors[j] * vectors[i], axis=1, keepdims=True) * solved[j]
        pivot = 0.5 * jnp.sum(vectors[i] * vectors[i], axis=1, keepdims=True)
        solved.append(value / pivot)
    return solved


def lay_pairs(vectors, pairs_ref):
    refl, (spans, band) = len(vectors), vectors[0].shape
    factors = span_factors(vectors)
    for i in range(refl):
        pairs_ref[:, i, 0:band] = vectors[i]
        pairs_ref[:, refl + i, 0:band] = factors[i]
        pairs_ref[:, i, band:] = jnp.zeros((spans, band), F32)
        pairs_ref[:, refl + i, band:] = jnp.zeros((spans, band), F32)


def window_of(begin, width):
    return pl.ds(pl.multiple_of(begin // LANE * LANE, LANE), width)


def apply_spans(begins, pairs, state_ref):
    refl, width = pairs[0].shape[0] // 2, pairs[0].shape[1]
    moved = [pltpu.roll(pair, begin % LANE, 1) for begin, pair in zip(begins, pairs)]
    windows = [state_ref[:, window_of(begin, width)] for begin in begins]
    inner = [
        [jnp.sum(window * pair[i : i + 1, :], axis=1, keepdims=True) for i in range(refl)]
        for window, pair in zip(windows, moved)
    ]
    for begin, window, pair, sums in zip(begins, windows, moved, inner):
        for i in range(refl):
            window = window - sums[i] * pair[refl + i : refl + i + 1, :]
        state_ref[:, window_of(begin, width)] = window


def apply_span(begin, pair, state_ref):
    apply_spans([begin], [pair], state_ref)


def apply_in_order(begins, pairs_ref, spots, state_ref):
    if len(begins) == 1:
        apply_span(begins[0], pairs_ref[spots[0]], state_ref)
        return
    tiles = [begin // LANE for begin in begins]
    apart = [
        jnp.abs(one - other) >= pairs_ref.shape[-1] // LANE
        for at, one in enumerate(tiles)
        for other in tiles[:at]
    ]
    clear = functools.reduce(jnp.logical_and, apart)

    @pl.when(clear)
    def _():
        apply_spans(begins, [pairs_ref[spot] for spot in spots], state_ref)

    @pl.when(jnp.logical_not(clear))
    def _():
        half = len(begins) // 2
        apply_in_order(begins[:half], pairs_ref, spots[:half], state_ref)
        apply_in_order(begins[half:], pairs_ref, spots[half:], state_ref)


def front_kernel(
    offsets_ref, vectors_ref, panels_ref, eigen_ref, *refs
):
    *piece_refs, down_out, up_out = refs[:6]
    down_ref, up_ref, wide_ref, sems = refs[6:]
    sweeps, spans, refl, band = vectors_ref.shape
    rows, columns = eigen_ref.shape
    panels, own, _ = panels_ref.shape
    moves = [
        pltpu.make_async_copy(
            panels_ref.at[p], wide_ref.at[p * own : (p + 1) * own, 0:columns], sems.at[p]
        )
        for p in range(panels)
    ]
    halos = ((down_ref, None, sweeps), (up_ref, 0, sweeps - 1))
    for ref, begin, count in halos:
        width = ref.shape[1] - count * band - LANE
        begin = columns - width if begin is None else begin
        moves.append(
            pltpu.make_async_copy(
                eigen_ref.at[:, begin : begin + width], ref.at[:, 0:width], sems.at[len(moves)]
            )
        )
    for move in moves:
        move.start()
    wide_ref[:, columns:] = jnp.zeros((panels * own, wide_ref.shape[1] - columns), BF16)
    for ref, _, count in halos:
        width = ref.shape[1] - count * band - LANE
        for sweep in range(count):
            for i in range(refl):
                ref[i * spans : (i + 1) * spans, width + sweep * band : width + (sweep + 1) * band] = (
                    vectors_ref[sweep, :, i, :]
                )
        ref[:, width + count * band :] = jnp.zeros((rows, LANE), F32)
        ref[0:sweeps, width + count * band : width + count * band + spans] = offsets_ref[...].astype(F32)
    for move in moves[:panels]:
        move.wait()
    leaves = []

    def leave(source, target):
        leaves.append(pltpu.make_async_copy(source, target, sems.at[len(moves) + len(leaves)]))
        leaves[-1].start()

    for step, ref in zip((0, *PEERS), piece_refs):
        cut = ref.shape[1]
        at = pl.multiple_of((lax.axis_index("x") + step) % X_SIZE * cut, LANE)
        leave(wide_ref.at[:, pl.ds(at, cut)], ref)
    for move, source, target in zip(moves[panels:], (down_ref, up_ref), (down_out, up_out)):
        move.wait()
        leave(source, target)
    for move in leaves:
        move.wait()


def halo_sizes(vectors):
    sweeps, spans, _, band = vectors.shape
    return sweeps * spans * band, ((sweeps - 1) * spans + 1) * band


def front(eigen, vectors, offsets, panels, cut):
    sweeps, _, _, band = vectors.shape
    rows = eigen.shape[0]
    left, right = halo_sizes(vectors)
    wide = lambda width: jax.ShapeDtypeStruct((rows, width), F32)
    high = panels.shape[0] * panels.shape[1]
    return call(
        front_kernel,
        [jax.ShapeDtypeStruct((high, cut), BF16)] * 4
        + [wide(left + sweeps * band + LANE), wide(right + (sweeps - 1) * band + LANE)],
        [VM, VM, ANY, ANY],
        (offsets, vectors, panels, eigen),
        [
            pltpu.VMEM((rows, left + sweeps * band + LANE), F32),
            pltpu.VMEM((rows, right + (sweeps - 1) * band + LANE), F32),
            pltpu.VMEM((high, X_SIZE * cut), BF16),
            pltpu.SemaphoreType.DMA((panels.shape[0] + 8,)),
        ],
        flops=panels.size,
        size=4 * panels.size,
        vmem=FRONT_MB,
        outs=[ANY] * 6,
    )


def sweep_kernel(
    offsets_ref, upper_offsets_ref, lower_offsets_ref,
    vectors_ref, own_ref, upper_ref, lower_ref,
    out_ref, mine_ref, next_ref, last_ref, one_ref, two_ref,
    state_ref, pairs_ref, rounded_ref,
):
    sweeps, spans, refl, band = vectors_ref.shape
    rows, columns = own_ref.shape
    left = upper_ref.shape[1] - sweeps * band - LANE
    right = lower_ref.shape[1] - (sweeps - 1) * band - LANE
    state_ref[:, 0:left] = upper_ref[:, 0:left]
    state_ref[:, left : left + columns] = own_ref[...]
    state_ref[:, left + columns :] = lower_ref[:, 0:right]
    first = lax.axis_index("row") == 0
    final = lax.axis_index("row") == lax.axis_size("row") - 1

    def beside(ref, width, sweep, i):
        return ref[i * spans : (i + 1) * spans, width + sweep * band : width + (sweep + 1) * band]

    for sweep in range(sweeps):
        lay_pairs([beside(upper_ref, left, sweep, i) for i in range(refl)], pairs_ref.at[sweep * 3])
        lay_pairs([vectors_ref[sweep, :, i, :] for i in range(refl)], pairs_ref.at[sweep * 3 + 1])
        if sweep < sweeps - 1:
            lay_pairs([beside(lower_ref, right, sweep, i) for i in range(refl)], pairs_ref.at[sweep * 3 + 2])
    for sweep in range(sweeps):

        def from_upper(at, carry, sweep=sweep):
            begin = upper_offsets_ref[sweep, at] - (columns - left)

            @pl.when(jnp.logical_and(begin >= 0, jnp.logical_not(first)))
            def _():
                apply_span(begin, pairs_ref[sweep * 3, at], state_ref)

            return carry

        def from_lower(at, carry, sweep=sweep):
            begin = lower_offsets_ref[sweep, at]

            @pl.when(jnp.logical_and(begin <= right - band, jnp.logical_not(final)))
            def _():
                apply_span(left + columns + begin, pairs_ref[sweep * 3 + 2, at], state_ref)

            return carry

        lax.fori_loop(0, spans, from_upper, 0)
        for at in range(0, spans, GROUP):
            group = range(at, at + GROUP)
            apply_in_order(
                [left + offsets_ref[sweep, k] for k in group],
                pairs_ref,
                [(sweep * 3 + 1, k) for k in group],
                state_ref,
            )
        if sweep < sweeps - 1:
            lax.fori_loop(0, spans, from_lower, 0)
    out_ref[...] = state_ref[:, left : left + columns]
    padded = rounded_ref.shape[1]
    rounded_ref[:, 0:columns] = state_ref[:, left : left + columns].astype(BF16)
    rounded_ref[:, columns:] = jnp.zeros((rows, padded - columns), BF16)
    cut = mine_ref.shape[1]
    half = rows // 2
    targets = (
        (0, 0, mine_ref), (PEERS[0], 0, next_ref), (PEERS[1], 0, last_ref),
        (PEERS[2], 0, one_ref), (PEERS[2], half, two_ref),
    )
    for step, row, ref in targets:
        at = pl.multiple_of((lax.axis_index("x") + step) % X_SIZE * cut, LANE)
        ref[...] = rounded_ref[row : row + ref.shape[0], pl.ds(at, cut)]


def sweep_all(eigen, vectors, offsets, down, up, cut):
    sweeps, spans, refl, band = vectors.shape
    rows, columns = eigen.shape
    left, right = halo_sizes(vectors)
    assert left + right + band < columns and spans * refl == rows
    upper = from_behind(down, "row", 1)
    lower = from_behind(up, "row", -1)
    upper_offsets = upper[0:sweeps, -LANE : spans - LANE].astype(jnp.int32)
    lower_offsets = lower[0:sweeps, -LANE : spans - LANE].astype(jnp.int32)
    return call(
        sweep_kernel,
        [jax.ShapeDtypeStruct(eigen.shape, F32)]
        + piece_shapes(rows, cut),
        [SM] * 3 + [VM] * 4,
        (offsets, upper_offsets, lower_offsets, vectors, eigen, upper, lower),
        [
            pltpu.VMEM((rows, left + columns + right), F32),
            pltpu.VMEM((3 * sweeps, spans, 2 * refl, 2 * band), F32),
            pltpu.VMEM((rows, X_SIZE * cut), BF16),
        ],
        flops=40 * eigen.size,
        size=12 * eigen.size,
        vmem=14,
    )


def piece_shapes(rows, cut):
    full, half = jax.ShapeDtypeStruct((rows, cut), BF16), jax.ShapeDtypeStruct((rows // 2, cut), BF16)
    return [full, full, full, half, half]


def traded(pieces):
    steps = (1, -1, 2) if len(pieces) == 4 else (1, -1, 2, -2)
    got = []
    for piece, step in zip(pieces[1:], steps):
        got.append(shifted(piece, "x", step))
    return got


def ring(block, far):
    ahead = behind = block
    found = [(0, block)]
    for step in range(1, Z_SIZE // 2):
        ahead = shifted(ahead, "z", 1)
        behind = shifted(behind, "z", -1)
        found += [(step, ahead), (Z_SIZE - step, behind)]
    found.append((Z_SIZE // 2, shifted(ahead if far > 0 else behind, "z", far)))
    return found


def products_kernel(*refs, spots, own, rows):
    blocks, (mine, one, two, half0, half1) = refs[: len(spots)], refs[len(spots) : len(spots) + 5]
    ordered_ref, sums_ref, eigen_ref = refs[len(spots) + 5 :]
    order = ordered_ref.shape[0]
    x, z = lax.axis_index("x"), lax.axis_index("z")
    for ref, units in zip(blocks, spots):
        for at, (back_z, back_x, panel) in enumerate(units):
            source = (x + X_SIZE - back_x) % X_SIZE * Z_SIZE + (z + Z_SIZE - back_z) % Z_SIZE
            to = pl.multiple_of(panel * (order // 2) + source * own, UNIT)
            ordered_ref[pl.ds(to, own), :] = ref[at * own : (at + 1) * own, :]
    sources = ((0, 0, mine), (1, 0, one), (3, 0, two), (2, 0, half0), (2, rows // 2, half1))
    for back, row, ref in sources:
        to = pl.multiple_of((x + X_SIZE - back) % X_SIZE * rows + row, UNIT)
        eigen_ref[pl.ds(to, ref.shape[0]), :] = ref[...]

    def put(value, at):
        sums_ref[at * LANE : (at + 1) * LANE] = value.astype(BF16)

    def dot(first, count, other):
        return lax.dot_general(
            ordered_ref[first : first + count, :], other, CONTRACT_LAST, preferred_element_type=F32
        )

    width = order // 2
    early = dot(0, order, ordered_ref[0:width, :])
    late = dot(width, width, ordered_ref[width:, :])
    inner = dot(0, order, eigen_ref[...])
    tile = lambda value, i, j: value[i * LANE : (i + 1) * LANE, j * LANE : (j + 1) * LANE]
    for i in range(4):
        put(tile(inner, i, 0), i)
    for at, (i, j) in enumerate(((0, 0), (0, 1), (1, 1), (2, 0), (2, 1), (3, 0), (3, 1))):
        put(tile(early, i, j), 4 + at)
    for at, (i, j) in enumerate(((0, 0), (0, 1), (1, 1))):
        put(tile(late, i, j), 11 + at)


TILES = {
    at: 4 + k
    for k, at in enumerate(
        ((0, 0), (0, 1), (1, 1), (2, 0), (2, 1), (3, 0), (3, 1), (2, 2), (2, 3), (3, 3))
    )
}


def products(found, pieces, spots, own, order, rows):
    cut = pieces[0].shape[1]
    return call(
        functools.partial(products_kernel, spots=spots, own=own, rows=rows),
        [
            jax.ShapeDtypeStruct((order, cut), BF16),
            jax.ShapeDtypeStruct(((4 + len(TILES)) * LANE, LANE), BF16),
        ],
        [VM] * (len(found) + len(pieces)),
        (*found, *pieces),
        [pltpu.VMEM((LANE, cut), BF16)],
        flops=2 * order * (order + LANE) * cut,
        size=6 * order * cut,
        vmem=18,
    )


def split(value):
    high = value.astype(BF16)
    return high, (value - high.astype(F32)).astype(BF16)


def fine_dot(a, b):
    a0, a1 = a if isinstance(a, tuple) else split(a)
    b0, b1 = b if isinstance(b, tuple) else split(b)
    dot = functools.partial(jnp.dot, preferred_element_type=F32)
    total = dot(a0, b0)
    if b1 is not None:
        total = total + dot(a0, b1)
    if a1 is not None:
        total = total + dot(a1, b0)
    return total


def small_inverses(grams):
    order = grams[0].shape[0]
    row = lax.broadcasted_iota(jnp.int32, (order, order), 0)
    col = lax.broadcasted_iota(jnp.int32, (order, order), 1)
    eye = row == col
    wide = [gram.astype(F32) for gram in grams]
    found = [jnp.where(eye, 2.0 / jnp.where(eye, gram, 1.0), 0.0) for gram in wide]
    size = 1
    while size < order:
        pick = (row // (2 * size) == col // (2 * size)) & (row // size < col // size)
        parts = [jnp.where(pick, gram, 0.0) for gram in wide]
        if size == 1:
            steps = [
                jnp.sum(f, axis=1, keepdims=True) * part * jnp.sum(f, axis=0, keepdims=True)
                for f, part in zip(found, parts)
            ]
        else:
            halves = [split(f) for f in found]
            steps = [fine_dot((part.astype(BF16), None), f) for part, f in zip(parts, halves)]
            steps = [fine_dot(f, step) for f, step in zip(halves, steps)]
        found = [f - step for f, step in zip(found, steps)]
        size *= 2
    return found


def correction_kernel(
    sums_ref, ordered_ref, mine_ref, next_ref, last_ref, one_ref, two_ref, coeffs_ref
):
    rows = mine_ref.shape[0]
    tile = lambda at: sums_ref[at * LANE : (at + 1) * LANE, :]
    gram = lambda i, j: tile(TILES[i, j])
    inverses = [split(f) for f in small_inverses([gram(i, i) for i in range(4)])]
    solved = {}
    for i in (1, 0, 3, 2):
        value = tile(i).astype(F32)
        for j in solved:
            if j // 2 < i // 2:
                known = (solved[j].astype(BF16), None)
            else:
                known = solved[j]
            value = value - fine_dot((gram(i, j), None), known)
        solved[i] = fine_dot(inverses[i], value)
        turned = solved[i].T.astype(BF16)
        for x in range(X_SIZE):
            to = pl.multiple_of((x + X_SIZE - lax.axis_index("x")) % X_SIZE * rows, UNIT)
            coeffs_ref[pl.ds(to, rows), i * LANE : (i + 1) * LANE] = turned[x * rows : (x + 1) * rows]
    product = jnp.dot(
        coeffs_ref[...], ordered_ref[...], preferred_element_type=F32
    ).astype(BF16)
    piece = lambda step: product[step * rows : (step + 1) * rows]
    mine_ref[...] = piece(0)
    next_ref[...] = piece(PEERS[0])
    last_ref[...] = piece(PEERS[1])
    one_ref[...] = piece(PEERS[2])[0 : rows // 2]
    two_ref[...] = piece(PEERS[2])[rows // 2 :]


def correction(sums, ordered, rows):
    order, cut = ordered.shape
    return call(
        correction_kernel,
        piece_shapes(rows, cut),
        [VM, VM],
        (sums, ordered),
        [pltpu.VMEM((LANE, order), BF16)],
        flops=2 * order * LANE * cut,
        size=4 * order * cut,
        vmem=24,
    )


def subtract_kernel(eigen_ref, mine, one, two, half0, half1, out_ref, held_ref, sems):
    rows, columns = eigen_ref.shape
    cut = mine.shape[1]
    half = rows // 2
    sources = {0: ((0, mine),), 1: ((0, one),), 3: ((0, two),), 2: ((0, half0), (half, half1))}
    leaves = []
    for at in range(X_SIZE):
        begin, span = at * cut, min(cut, columns - at * cut)
        for back, refs in sources.items():

            @pl.when((lax.axis_index("x") + X_SIZE - back) % X_SIZE == at)
            def _(refs=refs, begin=begin, span=span):
                for row, ref in refs:
                    high = row + ref.shape[0]
                    held_ref[row:high, begin : begin + span] = (
                        eigen_ref[row:high, begin : begin + span] - ref[:, 0:span].astype(F32)
                    )

        chunk = slice(begin, begin + span)
        leaves.append(
            pltpu.make_async_copy(held_ref.at[:, chunk], out_ref.at[:, chunk], sems.at[at])
        )
        leaves[-1].start()
    for leave in leaves:
        leave.wait()


def subtract(eigen, pieces):
    return call(
        subtract_kernel,
        jax.ShapeDtypeStruct(eigen.shape, F32),
        [VM] * 6,
        (eigen, *pieces),
        [pltpu.VMEM(eigen.shape, F32), pltpu.SemaphoreType.DMA((X_SIZE,))],
        flops=eigen.size,
        size=10 * eigen.size,
        vmem=12,
        outs=ANY,
    )


def total_kernel(parts_ref, out_ref):
    total = parts_ref[0].astype(F32)
    for at in range(1, parts_ref.shape[0]):
        total = total + parts_ref[at].astype(F32)
    total = total.astype(BF16)
    for at in range(parts_ref.shape[0]):
        out_ref[at] = total


def total_for_all(parts):
    return call(
        total_kernel,
        jax.ShapeDtypeStruct(parts.shape, BF16),
        [VM],
        (parts,),
        flops=parts.size,
        size=4 * parts.size,
        vmem=4,
    )


def exchange(pieces, axes):
    return lax.all_to_all(pieces, axes, 0, 0, tiled=True)


def inner(eigvecs, span_vectors, span_offsets, panels):
    assert (lax.axis_size("x"), lax.axis_size("z")) == (X_SIZE, Z_SIZE)
    peers = lax.axis_size("row") * X_SIZE
    count, own, columns = panels.shape
    rows = eigvecs.shape[0]
    order = count * own * X_SIZE * Z_SIZE
    cut = -(-columns // (LANE * X_SIZE)) * LANE
    *packed, down, up = front(eigvecs, span_vectors, span_offsets, panels, cut)
    swept = sweep_all(eigvecs, span_vectors, span_offsets, down, up, cut)
    eigen, pieces = swept[0], swept[1:]
    one, two, far = traded(packed)
    found, spots = [], []
    for at, (pair, sources) in enumerate((((packed[0], one), (0, 1)), ((two, far), (3, 2)))):
        unit = [(back_x, panel) for back_x in sources for panel in range(count)]
        for back, block in ring(jnp.concatenate(pair, axis=0), 1 - 2 * at):
            found.append(block)
            spots.append([(back, back_x, panel) for back_x, panel in unit])
    others = [pieces[0], *traded(pieces)]
    ordered, sums = products(found, others, spots, own, order, rows)

    parts = exchange(sums.reshape(peers, -1, LANE), ("row", "x"))
    sums = exchange(total_for_all(parts), ("row", "x"))
    corrections = correction(sums.reshape(-1, LANE), ordered, rows)
    return subtract(eigen, [corrections[0], *traded(corrections)])


def solution(mesh):
    finer = Mesh(
        mesh.devices.reshape(mesh.shape["row"], X_SIZE, Z_SIZE), ("row", "x", "z")
    )
    placed = (P(COL, "row"), P(None, "row", None, None), P(None, "row"), P(None, COL, "row"))
    return jax.shard_map(
        inner, mesh=finer, in_specs=placed, out_specs=P(COL, "row"), check_vma=False
    )
```

```python
import functools

import jax
import jax.numpy as jnp
from jax import lax
from jax.experimental import pallas as pl
from jax.experimental.pallas import tpu as pltpu
from jax.sharding import Mesh
from jax.sharding import PartitionSpec as P


COL = ("x", "z")
X_SIZE, Z_SIZE = 4, 8
LANE = 128
GROUP = 4
FRONT_MB = 60
UNIT = 8
F32 = jnp.float32
BF16 = jnp.bfloat16
CONTRACT_LAST = (((1,), (1,)), ((), ()))
VM = pl.BlockSpec(memory_space=pltpu.VMEM)
SM = pl.BlockSpec(memory_space=pltpu.SMEM)
ANY = pl.BlockSpec(memory_space=pl.ANY)
PEERS = (1, 3, 2)


def call(kernel, out_shape, in_specs, args, scratch=(), flops=0, size=0, vmem=0, outs=None):
    outs = outs or jax.tree.map(lambda _: VM, out_shape)
    return pl.pallas_call(
        kernel,
        out_shape=out_shape,
        in_specs=in_specs,
        out_specs=outs,
        scratch_shapes=list(scratch),
        compiler_params=pltpu.CompilerParams(vmem_limit_bytes=vmem << 20) if vmem else None,
        cost_estimate=pl.CostEstimate(flops=flops, bytes_accessed=size, transcendentals=0),
    )(*args)


def shifted(value, axis, steps):
    count = lax.axis_size(axis)
    return lax.ppermute(value, axis, [(at, (at + steps) % count) for at in range(count)])


def from_behind(value, axis, steps):
    count = lax.axis_size(axis)
    first, last = (max(0, -steps), min(count, count - steps))
    return lax.ppermute(value, axis, [(source, source + steps) for source in range(first, last)])


def span_factors(vectors):
    solved = []
    for i in range(len(vectors)):
        value = vectors[i]
        for j in range(i):
            value = value - jnp.sum(vectors[j] * vectors[i], axis=1, keepdims=True) * solved[j]
        pivot = 0.5 * jnp.sum(vectors[i] * vectors[i], axis=1, keepdims=True)
        solved.append(value / pivot)
    return solved


def lay_pairs(vectors, pairs_ref):
    refl, (spans, band) = len(vectors), vectors[0].shape
    factors = span_factors(vectors)
    for i in range(refl):
        pairs_ref[:, i, 0:band] = vectors[i]
        pairs_ref[:, refl + i, 0:band] = factors[i]
        pairs_ref[:, i, band:] = jnp.zeros((spans, band), F32)
        pairs_ref[:, refl + i, band:] = jnp.zeros((spans, band), F32)


def window_of(begin, width):
    return pl.ds(pl.multiple_of(begin // LANE * LANE, LANE), width)


def apply_spans(begins, pairs, state_ref):
    refl, width = pairs[0].shape[0] // 2, pairs[0].shape[1]
    moved = [pltpu.roll(pair, begin % LANE, 1) for begin, pair in zip(begins, pairs)]
    windows = [state_ref[:, window_of(begin, width)] for begin in begins]
    inner = [
        [jnp.sum(window * pair[i : i + 1, :], axis=1, keepdims=True) for i in range(refl)]
        for window, pair in zip(windows, moved)
    ]
    for begin, window, pair, sums in zip(begins, windows, moved, inner):
        for i in range(refl):
            window = window - sums[i] * pair[refl + i : refl + i + 1, :]
        state_ref[:, window_of(begin, width)] = window


def apply_span(begin, pair, state_ref):
    apply_spans([begin], [pair], state_ref)


def apply_in_order(begins, pairs_ref, spots, state_ref):
    if len(begins) == 1:
        apply_span(begins[0], pairs_ref[spots[0]], state_ref)
        return
    tiles = [begin // LANE for begin in begins]
    apart = [
        jnp.abs(one - other) >= pairs_ref.shape[-1] // LANE
        for at, one in enumerate(tiles)
        for other in tiles[:at]
    ]
    clear = functools.reduce(jnp.logical_and, apart)

    @pl.when(clear)
    def _():
        apply_spans(begins, [pairs_ref[spot] for spot in spots], state_ref)

    @pl.when(jnp.logical_not(clear))
    def _():
        half = len(begins) // 2
        apply_in_order(begins[:half], pairs_ref, spots[:half], state_ref)
        apply_in_order(begins[half:], pairs_ref, spots[half:], state_ref)


def front_kernel(
    offsets_ref, vectors_ref, panels_ref, eigen_ref, *refs
):
    *piece_refs, down_out, up_out = refs[:6]
    down_ref, up_ref, wide_ref, held_vectors_ref, held_offsets_ref, sems = refs[6:]
    sweeps, spans, refl, band = vectors_ref.shape
    rows, columns = eigen_ref.shape
    panels, own, _ = panels_ref.shape
    moves = [
        pltpu.make_async_copy(
            panels_ref.at[p], wide_ref.at[p * own : (p + 1) * own, 0:columns], sems.at[p]
        )
        for p in range(panels)
    ]
    halos = ((down_ref, None, sweeps), (up_ref, 0, sweeps - 1))
    for ref, begin, count in halos:
        width = ref.shape[1] - count * band - LANE
        begin = columns - width if begin is None else begin
        moves.append(
            pltpu.make_async_copy(
                eigen_ref.at[:, begin : begin + width], ref.at[:, 0:width], sems.at[len(moves)]
            )
        )
    small = [
        pltpu.make_async_copy(vectors_ref, held_vectors_ref, sems.at[len(moves)]),
        pltpu.make_async_copy(offsets_ref, held_offsets_ref, sems.at[len(moves) + 1]),
    ]
    for move in moves + small:
        move.start()
    wide_ref[:, columns:] = jnp.zeros((panels * own, wide_ref.shape[1] - columns), BF16)
    leaves = []

    def leave(source, target):
        leaves.append(pltpu.make_async_copy(source, target, sems.at[len(moves) + 2 + len(leaves)]))
        leaves[-1].start()

    for move in moves[:panels]:
        move.wait()
    for step, ref in zip((*PEERS, 0), (*piece_refs[1:], piece_refs[0])):
        cut = ref.shape[1]
        at = pl.multiple_of((lax.axis_index("x") + step) % X_SIZE * cut, LANE)
        leave(wide_ref.at[:, pl.ds(at, cut)], ref)
    for move in small:
        move.wait()
    for ref, _, count in halos:
        width = ref.shape[1] - count * band - LANE
        for sweep in range(count):
            for i in range(refl):
                ref[i * spans : (i + 1) * spans, width + sweep * band : width + (sweep + 1) * band] = (
                    held_vectors_ref[sweep, :, i, :]
                )
        ref[:, width + count * band :] = jnp.zeros((rows, LANE), F32)
        starts = held_offsets_ref[...].astype(F32)
        ref[0:sweeps, width + count * band : width + count * band + spans] = starts
    for move, source, target in zip(moves[panels:], (down_ref, up_ref), (down_out, up_out)):
        move.wait()
        leave(source, target)
    for move in leaves:
        move.wait()


def halo_sizes(vectors):
    sweeps, spans, _, band = vectors.shape
    return sweeps * spans * band, ((sweeps - 1) * spans + 1) * band


def front(eigen, vectors, offsets, panels, cut):
    sweeps, _, _, band = vectors.shape
    rows = eigen.shape[0]
    left, right = halo_sizes(vectors)
    wide = lambda width: jax.ShapeDtypeStruct((rows, width), F32)
    high = panels.shape[0] * panels.shape[1]
    return call(
        front_kernel,
        [jax.ShapeDtypeStruct((high, cut), BF16)] * 4
        + [wide(left + sweeps * band + LANE), wide(right + (sweeps - 1) * band + LANE)],
        [ANY] * 4,
        (offsets, vectors, panels, eigen),
        [
            pltpu.VMEM((rows, left + sweeps * band + LANE), F32),
            pltpu.VMEM((rows, right + (sweeps - 1) * band + LANE), F32),
            pltpu.VMEM((high, X_SIZE * cut), BF16),
            pltpu.VMEM(vectors.shape, F32),
            pltpu.VMEM(offsets.shape, jnp.int32),
            pltpu.SemaphoreType.DMA((panels.shape[0] + 10,)),
        ],
        flops=panels.size,
        size=4 * panels.size,
        vmem=FRONT_MB,
        outs=[ANY] * 6,
    )


def sweep_kernel(
    offsets_ref, upper_offsets_ref, lower_offsets_ref,
    vectors_ref, own_ref, upper_ref, lower_ref,
    out_ref, mine_ref, next_ref, last_ref, one_ref, two_ref,
    state_ref, pairs_ref, rounded_ref,
):
    sweeps, spans, refl, band = vectors_ref.shape
    rows, columns = own_ref.shape
    left = upper_ref.shape[1] - sweeps * band - LANE
    right = lower_ref.shape[1] - (sweeps - 1) * band - LANE
    state_ref[:, 0:left] = upper_ref[:, 0:left]
    state_ref[:, left : left + columns] = own_ref[...]
    state_ref[:, left + columns :] = lower_ref[:, 0:right]
    first = lax.axis_index("row") == 0
    final = lax.axis_index("row") == lax.axis_size("row") - 1

    def beside(ref, width, sweep, i):
        return ref[i * spans : (i + 1) * spans, width + sweep * band : width + (sweep + 1) * band]

    for sweep in range(sweeps):
        lay_pairs([beside(upper_ref, left, sweep, i) for i in range(refl)], pairs_ref.at[sweep * 3])
        lay_pairs([vectors_ref[sweep, :, i, :] for i in range(refl)], pairs_ref.at[sweep * 3 + 1])
        if sweep < sweeps - 1:
            lay_pairs([beside(lower_ref, right, sweep, i) for i in range(refl)], pairs_ref.at[sweep * 3 + 2])
    for sweep in range(sweeps):

        def from_upper(at, carry, sweep=sweep):
            begin = upper_offsets_ref[sweep, at] - (columns - left)

            @pl.when(jnp.logical_and(begin >= 0, jnp.logical_not(first)))
            def _():
                apply_span(begin, pairs_ref[sweep * 3, at], state_ref)

            return carry

        def from_lower(at, carry, sweep=sweep):
            begin = lower_offsets_ref[sweep, at]

            @pl.when(jnp.logical_and(begin <= right - band, jnp.logical_not(final)))
            def _():
                apply_span(left + columns + begin, pairs_ref[sweep * 3 + 2, at], state_ref)

            return carry

        lax.fori_loop(0, spans, from_upper, 0)
        for at in range(0, spans, GROUP):
            group = range(at, at + GROUP)
            apply_in_order(
                [left + offsets_ref[sweep, k] for k in group],
                pairs_ref,
                [(sweep * 3 + 1, k) for k in group],
                state_ref,
            )
        if sweep < sweeps - 1:
            lax.fori_loop(0, spans, from_lower, 0)
    out_ref[...] = state_ref[:, left : left + columns]
    padded = rounded_ref.shape[1]
    rounded_ref[:, 0:columns] = state_ref[:, left : left + columns].astype(BF16)
    rounded_ref[:, columns:] = jnp.zeros((rows, padded - columns), BF16)
    cut = mine_ref.shape[1]
    half = rows // 2
    targets = (
        (0, 0, mine_ref), (PEERS[0], 0, next_ref), (PEERS[1], 0, last_ref),
        (PEERS[2], 0, one_ref), (PEERS[2], half, two_ref),
    )
    for step, row, ref in targets:
        at = pl.multiple_of((lax.axis_index("x") + step) % X_SIZE * cut, LANE)
        ref[...] = rounded_ref[row : row + ref.shape[0], pl.ds(at, cut)]


def sweep_all(eigen, vectors, offsets, down, up, cut):
    sweeps, spans, refl, band = vectors.shape
    rows, columns = eigen.shape
    left, right = halo_sizes(vectors)
    assert left + right + band < columns and spans * refl == rows
    upper = from_behind(down, "row", 1)
    lower = from_behind(up, "row", -1)
    upper_offsets = upper[0:sweeps, -LANE : spans - LANE].astype(jnp.int32)
    lower_offsets = lower[0:sweeps, -LANE : spans - LANE].astype(jnp.int32)
    return call(
        sweep_kernel,
        [jax.ShapeDtypeStruct(eigen.shape, F32)]
        + piece_shapes(rows, cut),
        [SM] * 3 + [VM] * 4,
        (offsets, upper_offsets, lower_offsets, vectors, eigen, upper, lower),
        [
            pltpu.VMEM((rows, left + columns + right), F32),
            pltpu.VMEM((3 * sweeps, spans, 2 * refl, 2 * band), F32),
            pltpu.VMEM((rows, X_SIZE * cut), BF16),
        ],
        flops=40 * eigen.size,
        size=12 * eigen.size,
        vmem=14,
    )


def piece_shapes(rows, cut):
    full, half = jax.ShapeDtypeStruct((rows, cut), BF16), jax.ShapeDtypeStruct((rows // 2, cut), BF16)
    return [full, full, full, half, half]


def traded(pieces):
    steps = (1, -1, 2) if len(pieces) == 4 else (1, -1, 2, -2)
    got = []
    for piece, step in zip(pieces[1:], steps):
        got.append(shifted(piece, "x", step))
    return got


def ring(block, far):
    ahead = behind = block
    found = [(0, block)]
    for step in range(1, Z_SIZE // 2):
        ahead = shifted(ahead, "z", 1)
        behind = shifted(behind, "z", -1)
        found += [(step, ahead), (Z_SIZE - step, behind)]
    found.append((Z_SIZE // 2, shifted(ahead if far > 0 else behind, "z", far)))
    return found


def products_kernel(*refs, spots, own, rows):
    blocks, (mine, one, two, half0, half1) = refs[: len(spots)], refs[len(spots) : len(spots) + 5]
    ordered_ref, sums_ref, eigen_ref = refs[len(spots) + 5 :]
    order = ordered_ref.shape[0]
    x, z = lax.axis_index("x"), lax.axis_index("z")
    for ref, units in zip(blocks, spots):
        for at, (back_z, back_x, panel) in enumerate(units):
            source = (x + X_SIZE - back_x) % X_SIZE * Z_SIZE + (z + Z_SIZE - back_z) % Z_SIZE
            to = pl.multiple_of(panel * (order // 2) + source * own, UNIT)
            ordered_ref[pl.ds(to, own), :] = ref[at * own : (at + 1) * own, :]
    sources = ((0, 0, mine), (1, 0, one), (3, 0, two), (2, 0, half0), (2, rows // 2, half1))
    for back, row, ref in sources:
        to = pl.multiple_of((x + X_SIZE - back) % X_SIZE * rows + row, UNIT)
        eigen_ref[pl.ds(to, ref.shape[0]), :] = ref[...]

    def put(value, at):
        sums_ref[at * LANE : (at + 1) * LANE] = value.astype(BF16)

    def dot(first, count, other):
        return lax.dot_general(
            ordered_ref[first : first + count, :], other, CONTRACT_LAST, preferred_element_type=F32
        )

    width = order // 2
    early = dot(0, order, ordered_ref[0:width, :])
    late = dot(width, width, ordered_ref[width:, :])
    inner = dot(0, order, eigen_ref[...])
    tile = lambda value, i, j: value[i * LANE : (i + 1) * LANE, j * LANE : (j + 1) * LANE]
    for i in range(4):
        put(tile(inner, i, 0), i)
    for at, (i, j) in enumerate(((0, 0), (0, 1), (1, 1), (2, 0), (2, 1), (3, 0), (3, 1))):
        put(tile(early, i, j), 4 + at)
    for at, (i, j) in enumerate(((0, 0), (0, 1), (1, 1))):
        put(tile(late, i, j), 11 + at)


TILES = {
    at: 4 + k
    for k, at in enumerate(
        ((0, 0), (0, 1), (1, 1), (2, 0), (2, 1), (3, 0), (3, 1), (2, 2), (2, 3), (3, 3))
    )
}


def products(found, pieces, spots, own, order, rows):
    cut = pieces[0].shape[1]
    return call(
        functools.partial(products_kernel, spots=spots, own=own, rows=rows),
        [
            jax.ShapeDtypeStruct((order, cut), BF16),
            jax.ShapeDtypeStruct(((4 + len(TILES)) * LANE, LANE), BF16),
        ],
        [VM] * (len(found) + len(pieces)),
        (*found, *pieces),
        [pltpu.VMEM((LANE, cut), BF16)],
        flops=2 * order * (order + LANE) * cut,
        size=6 * order * cut,
        vmem=18,
    )


def split(value):
    high = value.astype(BF16)
    return high, (value - high.astype(F32)).astype(BF16)


def fine_dot(a, b):
    a0, a1 = a if isinstance(a, tuple) else split(a)
    b0, b1 = b if isinstance(b, tuple) else split(b)
    dot = functools.partial(jnp.dot, preferred_element_type=F32)
    total = dot(a0, b0)
    if b1 is not None:
        total = total + dot(a0, b1)
    if a1 is not None:
        total = total + dot(a1, b0)
    return total


def small_inverses(grams):
    order = grams[0].shape[0]
    row = lax.broadcasted_iota(jnp.int32, (order, order), 0)
    col = lax.broadcasted_iota(jnp.int32, (order, order), 1)
    eye = row == col
    wide = [gram.astype(F32) for gram in grams]
    found = [jnp.where(eye, 2.0 / jnp.where(eye, gram, 1.0), 0.0) for gram in wide]
    size = 1
    while size < order:
        pick = (row // (2 * size) == col // (2 * size)) & (row // size < col // size)
        parts = [jnp.where(pick, gram, 0.0) for gram in wide]
        if size == 1:
            steps = [
                jnp.sum(f, axis=1, keepdims=True) * part * jnp.sum(f, axis=0, keepdims=True)
                for f, part in zip(found, parts)
            ]
        else:
            halves = [split(f) for f in found]
            steps = [fine_dot((part.astype(BF16), None), f) for part, f in zip(parts, halves)]
            steps = [fine_dot(f, step) for f, step in zip(halves, steps)]
        found = [f - step for f, step in zip(found, steps)]
        size *= 2
    return found


def correction_kernel(
    sums_ref, ordered_ref, mine_ref, next_ref, last_ref, one_ref, two_ref, coeffs_ref
):
    rows = mine_ref.shape[0]
    tile = lambda at: sums_ref[at * LANE : (at + 1) * LANE, :]
    gram = lambda i, j: tile(TILES[i, j])
    inverses = [split(f) for f in small_inverses([gram(i, i) for i in range(4)])]
    above = [
        split(fine_dot(inverses[at], fine_dot((gram(at, at + 1), None), inverses[at + 1])))
        for at in (0, 2)
    ]

    def solve(panel, first, second):
        at = 2 * panel
        return [
            fine_dot(inverses[at], first) - fine_dot(above[panel], second),
            fine_dot(inverses[at + 1], second),
        ]

    solved = solve(0, (tile(0), None), (tile(1), None))
    known = [value.astype(BF16) for value in solved]
    rest = [
        tile(i).astype(F32)
        - jnp.dot(gram(i, 0), known[0], preferred_element_type=F32)
        - jnp.dot(gram(i, 1), known[1], preferred_element_type=F32)
        for i in (2, 3)
    ]
    solved += solve(1, *map(split, rest))
    for i in range(4):
        turned = solved[i].T.astype(BF16)
        for x in range(X_SIZE):
            to = pl.multiple_of((x + X_SIZE - lax.axis_index("x")) % X_SIZE * rows, UNIT)
            coeffs_ref[pl.ds(to, rows), i * LANE : (i + 1) * LANE] = turned[x * rows : (x + 1) * rows]
    product = jnp.dot(
        coeffs_ref[...], ordered_ref[...], preferred_element_type=F32
    ).astype(BF16)
    piece = lambda step: product[step * rows : (step + 1) * rows]
    mine_ref[...] = piece(0)
    next_ref[...] = piece(PEERS[0])
    last_ref[...] = piece(PEERS[1])
    one_ref[...] = piece(PEERS[2])[0 : rows // 2]
    two_ref[...] = piece(PEERS[2])[rows // 2 :]


def correction(sums, ordered, rows):
    order, cut = ordered.shape
    return call(
        correction_kernel,
        piece_shapes(rows, cut),
        [VM, VM],
        (sums, ordered),
        [pltpu.VMEM((LANE, order), BF16)],
        flops=2 * order * LANE * cut,
        size=4 * order * cut,
        vmem=24,
    )


def subtract_kernel(eigen_ref, mine, one, two, half0, half1, out_ref, held_ref, sems):
    rows, columns = eigen_ref.shape
    cut = mine.shape[1]
    half = rows // 2
    sources = {0: ((0, mine),), 1: ((0, one),), 3: ((0, two),), 2: ((0, half0), (half, half1))}
    leaves = []
    for at in range(X_SIZE):
        begin, span = at * cut, min(cut, columns - at * cut)
        for back, refs in sources.items():

            @pl.when((lax.axis_index("x") + X_SIZE - back) % X_SIZE == at)
            def _(refs=refs, begin=begin, span=span):
                for row, ref in refs:
                    high = row + ref.shape[0]
                    held_ref[row:high, begin : begin + span] = (
                        eigen_ref[row:high, begin : begin + span] - ref[:, 0:span].astype(F32)
                    )

        chunk = slice(begin, begin + span)
        leaves.append(
            pltpu.make_async_copy(held_ref.at[:, chunk], out_ref.at[:, chunk], sems.at[at])
        )
        leaves[-1].start()
    for leave in leaves:
        leave.wait()


def subtract(eigen, pieces):
    return call(
        subtract_kernel,
        jax.ShapeDtypeStruct(eigen.shape, F32),
        [VM] * 6,
        (eigen, *pieces),
        [pltpu.VMEM(eigen.shape, F32), pltpu.SemaphoreType.DMA((X_SIZE,))],
        flops=eigen.size,
        size=10 * eigen.size,
        vmem=12,
        outs=ANY,
    )


def total_kernel(parts_ref, out_ref):
    total = parts_ref[0].astype(F32)
    for at in range(1, parts_ref.shape[0]):
        total = total + parts_ref[at].astype(F32)
    total = total.astype(BF16)
    for at in range(parts_ref.shape[0]):
        out_ref[at] = total


def total_for_all(parts):
    return call(
        total_kernel,
        jax.ShapeDtypeStruct(parts.shape, BF16),
        [VM],
        (parts,),
        flops=parts.size,
        size=4 * parts.size,
        vmem=4,
    )


def exchange(pieces, axes):
    return lax.all_to_all(pieces, axes, 0, 0, tiled=True)


def inner(eigvecs, span_vectors, span_offsets, panels):
    assert (lax.axis_size("x"), lax.axis_size("z")) == (X_SIZE, Z_SIZE)
    peers = lax.axis_size("row") * X_SIZE
    count, own, columns = panels.shape
    rows = eigvecs.shape[0]
    order = count * own * X_SIZE * Z_SIZE
    cut = -(-columns // (LANE * X_SIZE)) * LANE
    *packed, down, up = front(eigvecs, span_vectors, span_offsets, panels, cut)
    swept = sweep_all(eigvecs, span_vectors, span_offsets, down, up, cut)
    eigen, pieces = swept[0], swept[1:]
    one, two, far = traded(packed)
    found, spots = [], []
    for at, (pair, sources) in enumerate((((packed[0], one), (0, 1)), ((two, far), (3, 2)))):
        unit = [(back_x, panel) for back_x in sources for panel in range(count)]
        for back, block in ring(jnp.concatenate(pair, axis=0), 1 - 2 * at):
            found.append(block)
            spots.append([(back, back_x, panel) for back_x, panel in unit])
    others = [pieces[0], *traded(pieces)]
    ordered, sums = products(found, others, spots, own, order, rows)

    parts = exchange(sums.reshape(peers, -1, LANE), ("row", "x"))
    sums = exchange(total_for_all(parts), ("row", "x"))
    corrections = correction(sums.reshape(-1, LANE), ordered, rows)
    return subtract(eigen, [corrections[0], *traded(corrections)])


def solution(mesh):
    finer = Mesh(
        mesh.devices.reshape(mesh.shape["row"], X_SIZE, Z_SIZE), ("row", "x", "z")
    )
    placed = (P(COL, "row"), P(None, "row", None, None), P(None, "row"), P(None, COL, "row"))
    return jax.shard_map(
        inner, mesh=finer, in_specs=placed, out_specs=P(COL, "row"), check_vma=False
    )
```

```python
import functools

import jax
import jax.numpy as jnp
from jax import lax
from jax.experimental import pallas as pl
from jax.experimental.pallas import tpu as pltpu
from jax.sharding import Mesh
from jax.sharding import PartitionSpec as P


COL = ("x", "z")
ROW = ("y", "core")
SUM_AXES = ("core", "x", "y")
X_SIZE, Z_SIZE = 4, 8
LANE = 128
GROUP = 4
FRONT_MB = 60
UNIT = 8
F32 = jnp.float32
BF16 = jnp.bfloat16
CONTRACT_LAST = (((1,), (1,)), ((), ()))
VM = pl.BlockSpec(memory_space=pltpu.VMEM)
SM = pl.BlockSpec(memory_space=pltpu.SMEM)
ANY = pl.BlockSpec(memory_space=pl.ANY)
PEERS = (1, 3, 2)


def call(kernel, out_shape, in_specs, args, scratch=(), flops=0, size=0, vmem=0, outs=None):
    outs = outs or jax.tree.map(lambda _: VM, out_shape)
    return pl.pallas_call(
        kernel,
        out_shape=out_shape,
        in_specs=in_specs,
        out_specs=outs,
        scratch_shapes=list(scratch),
        compiler_params=pltpu.CompilerParams(vmem_limit_bytes=vmem << 20) if vmem else None,
        cost_estimate=pl.CostEstimate(flops=flops, bytes_accessed=size, transcendentals=0),
    )(*args)


def shifted(value, axis, steps):
    count = lax.axis_size(axis)
    return lax.ppermute(value, axis, [(at, (at + steps) % count) for at in range(count)])


def from_behind(value, axis, steps):
    count = lax.axis_size(axis)
    first, last = (max(0, -steps), min(count, count - steps))
    return lax.ppermute(value, axis, [(source, source + steps) for source in range(first, last)])


def span_factors(vectors):
    solved = []
    for i in range(len(vectors)):
        value = vectors[i]
        for j in range(i):
            value = value - jnp.sum(vectors[j] * vectors[i], axis=1, keepdims=True) * solved[j]
        pivot = 0.5 * jnp.sum(vectors[i] * vectors[i], axis=1, keepdims=True)
        solved.append(value / pivot)
    return solved


def lay_pairs(vectors, pairs_ref):
    refl, (spans, band) = len(vectors), vectors[0].shape
    factors = span_factors(vectors)
    for i in range(refl):
        pairs_ref[:, i, 0:band] = vectors[i]
        pairs_ref[:, refl + i, 0:band] = factors[i]
        pairs_ref[:, i, band:] = jnp.zeros((spans, band), F32)
        pairs_ref[:, refl + i, band:] = jnp.zeros((spans, band), F32)


def window_of(begin, width):
    return pl.ds(pl.multiple_of(begin // LANE * LANE, LANE), width)


def apply_spans(begins, pairs, state_ref):
    refl, width = pairs[0].shape[0] // 2, pairs[0].shape[1]
    moved = [pltpu.roll(pair, begin % LANE, 1) for begin, pair in zip(begins, pairs)]
    windows = [state_ref[:, window_of(begin, width)] for begin in begins]
    inner = [
        [jnp.sum(window * pair[i : i + 1, :], axis=1, keepdims=True) for i in range(refl)]
        for window, pair in zip(windows, moved)
    ]
    for begin, window, pair, sums in zip(begins, windows, moved, inner):
        for i in range(refl):
            window = window - sums[i] * pair[refl + i : refl + i + 1, :]
        state_ref[:, window_of(begin, width)] = window


def apply_span(begin, pair, state_ref):
    apply_spans([begin], [pair], state_ref)


def apply_in_order(begins, pairs_ref, spots, state_ref):
    if len(begins) == 1:
        apply_span(begins[0], pairs_ref[spots[0]], state_ref)
        return
    tiles = [begin // LANE for begin in begins]
    apart = [
        jnp.abs(one - other) >= pairs_ref.shape[-1] // LANE
        for at, one in enumerate(tiles)
        for other in tiles[:at]
    ]
    clear = functools.reduce(jnp.logical_and, apart)

    @pl.when(clear)
    def _():
        apply_spans(begins, [pairs_ref[spot] for spot in spots], state_ref)

    @pl.when(jnp.logical_not(clear))
    def _():
        half = len(begins) // 2
        apply_in_order(begins[:half], pairs_ref, spots[:half], state_ref)
        apply_in_order(begins[half:], pairs_ref, spots[half:], state_ref)


def front_kernel(
    offsets_ref, vectors_ref, panels_ref, eigen_ref, *refs
):
    *piece_refs, down_out, up_out = refs[:6]
    down_ref, up_ref, wide_ref, held_vectors_ref, held_offsets_ref, sems = refs[6:]
    sweeps, spans, refl, band = vectors_ref.shape
    rows, columns = eigen_ref.shape
    panels, own, _ = panels_ref.shape
    moves = [
        pltpu.make_async_copy(
            panels_ref.at[p], wide_ref.at[p * own : (p + 1) * own, 0:columns], sems.at[p]
        )
        for p in range(panels)
    ]
    halos = ((down_ref, None, sweeps), (up_ref, 0, sweeps - 1))
    for ref, begin, count in halos:
        width = ref.shape[1] - count * band - LANE
        begin = columns - width if begin is None else begin
        moves.append(
            pltpu.make_async_copy(
                eigen_ref.at[:, begin : begin + width], ref.at[:, 0:width], sems.at[len(moves)]
            )
        )
    small = [
        pltpu.make_async_copy(vectors_ref, held_vectors_ref, sems.at[len(moves)]),
        pltpu.make_async_copy(offsets_ref, held_offsets_ref, sems.at[len(moves) + 1]),
    ]
    for move in moves + small:
        move.start()
    wide_ref[:, columns:] = jnp.zeros((panels * own, wide_ref.shape[1] - columns), BF16)
    leaves = []

    def leave(source, target):
        leaves.append(pltpu.make_async_copy(source, target, sems.at[len(moves) + 2 + len(leaves)]))
        leaves[-1].start()

    for move in moves[:panels]:
        move.wait()
    for step, ref in zip((*PEERS, 0), (*piece_refs[1:], piece_refs[0])):
        cut = ref.shape[1]
        at = pl.multiple_of((lax.axis_index("x") + step) % X_SIZE * cut, LANE)
        leave(wide_ref.at[:, pl.ds(at, cut)], ref)
    for move in small:
        move.wait()
    for ref, _, count in halos:
        width = ref.shape[1] - count * band - LANE
        for sweep in range(count):
            for i in range(refl):
                ref[i * spans : (i + 1) * spans, width + sweep * band : width + (sweep + 1) * band] = (
                    held_vectors_ref[sweep, :, i, :]
                )
        ref[:, width + count * band :] = jnp.zeros((rows, LANE), F32)
        starts = held_offsets_ref[...].astype(F32)
        ref[0:sweeps, width + count * band : width + count * band + spans] = starts
    for move, source, target in zip(moves[panels:], (down_ref, up_ref), (down_out, up_out)):
        move.wait()
        leave(source, target)
    for move in leaves:
        move.wait()


def halo_sizes(vectors):
    sweeps, spans, _, band = vectors.shape
    return sweeps * spans * band, ((sweeps - 1) * spans + 1) * band


def front(eigen, vectors, offsets, panels, cut):
    sweeps, _, _, band = vectors.shape
    rows = eigen.shape[0]
    left, right = halo_sizes(vectors)
    wide = lambda width: jax.ShapeDtypeStruct((rows, width), F32)
    high = panels.shape[0] * panels.shape[1]
    return call(
        front_kernel,
        [jax.ShapeDtypeStruct((high, cut), BF16)] * 4
        + [wide(left + sweeps * band + LANE), wide(right + (sweeps - 1) * band + LANE)],
        [ANY] * 4,
        (offsets, vectors, panels, eigen),
        [
            pltpu.VMEM((rows, left + sweeps * band + LANE), F32),
            pltpu.VMEM((rows, right + (sweeps - 1) * band + LANE), F32),
            pltpu.VMEM((high, X_SIZE * cut), BF16),
            pltpu.VMEM(vectors.shape, F32),
            pltpu.VMEM(offsets.shape, jnp.int32),
            pltpu.SemaphoreType.DMA((panels.shape[0] + 10,)),
        ],
        flops=panels.size,
        size=4 * panels.size,
        vmem=FRONT_MB,
        outs=[ANY] * 6,
    )


def sweep_kernel(
    offsets_ref, upper_offsets_ref, lower_offsets_ref,
    vectors_ref, own_ref, upper_ref, lower_ref,
    out_ref, mine_ref, next_ref, last_ref, one_ref, two_ref,
    state_ref, pairs_ref, rounded_ref,
):
    sweeps, spans, refl, band = vectors_ref.shape
    rows, columns = own_ref.shape
    left = upper_ref.shape[1] - sweeps * band - LANE
    right = lower_ref.shape[1] - (sweeps - 1) * band - LANE
    state_ref[:, 0:left] = upper_ref[:, 0:left]
    state_ref[:, left : left + columns] = own_ref[...]
    state_ref[:, left + columns :] = lower_ref[:, 0:right]
    first = lax.axis_index(ROW) == 0
    final = lax.axis_index(ROW) == lax.axis_size(ROW) - 1

    def beside(ref, width, sweep, i):
        return ref[i * spans : (i + 1) * spans, width + sweep * band : width + (sweep + 1) * band]

    for sweep in range(sweeps):
        lay_pairs([beside(upper_ref, left, sweep, i) for i in range(refl)], pairs_ref.at[sweep * 3])
        lay_pairs([vectors_ref[sweep, :, i, :] for i in range(refl)], pairs_ref.at[sweep * 3 + 1])
        if sweep < sweeps - 1:
            lay_pairs([beside(lower_ref, right, sweep, i) for i in range(refl)], pairs_ref.at[sweep * 3 + 2])
    for sweep in range(sweeps):

        def from_upper(at, carry, sweep=sweep):
            begin = upper_offsets_ref[sweep, at] - (columns - left)

            @pl.when(jnp.logical_and(begin >= 0, jnp.logical_not(first)))
            def _():
                apply_span(begin, pairs_ref[sweep * 3, at], state_ref)

            return carry

        def from_lower(at, carry, sweep=sweep):
            begin = lower_offsets_ref[sweep, at]

            @pl.when(jnp.logical_and(begin <= right - band, jnp.logical_not(final)))
            def _():
                apply_span(left + columns + begin, pairs_ref[sweep * 3 + 2, at], state_ref)

            return carry

        lax.fori_loop(0, spans, from_upper, 0)
        for at in range(0, spans, GROUP):
            group = range(at, at + GROUP)
            apply_in_order(
                [left + offsets_ref[sweep, k] for k in group],
                pairs_ref,
                [(sweep * 3 + 1, k) for k in group],
                state_ref,
            )
        if sweep < sweeps - 1:
            lax.fori_loop(0, spans, from_lower, 0)
    out_ref[...] = state_ref[:, left : left + columns]
    padded = rounded_ref.shape[1]
    rounded_ref[:, 0:columns] = state_ref[:, left : left + columns].astype(BF16)
    rounded_ref[:, columns:] = jnp.zeros((rows, padded - columns), BF16)
    cut = mine_ref.shape[1]
    half = rows // 2
    targets = (
        (0, 0, mine_ref), (PEERS[0], 0, next_ref), (PEERS[1], 0, last_ref),
        (PEERS[2], 0, one_ref), (PEERS[2], half, two_ref),
    )
    for step, row, ref in targets:
        at = pl.multiple_of((lax.axis_index("x") + step) % X_SIZE * cut, LANE)
        ref[...] = rounded_ref[row : row + ref.shape[0], pl.ds(at, cut)]


def sweep_all(eigen, vectors, offsets, down, up, cut):
    sweeps, spans, refl, band = vectors.shape
    rows, columns = eigen.shape
    left, right = halo_sizes(vectors)
    assert left + right + band < columns and spans * refl == rows
    upper = from_behind(down, ROW, 1)
    lower = from_behind(up, ROW, -1)
    upper_offsets = upper[0:sweeps, -LANE : spans - LANE].astype(jnp.int32)
    lower_offsets = lower[0:sweeps, -LANE : spans - LANE].astype(jnp.int32)
    return call(
        sweep_kernel,
        [jax.ShapeDtypeStruct(eigen.shape, F32)]
        + piece_shapes(rows, cut),
        [SM] * 3 + [VM] * 4,
        (offsets, upper_offsets, lower_offsets, vectors, eigen, upper, lower),
        [
            pltpu.VMEM((rows, left + columns + right), F32),
            pltpu.VMEM((3 * sweeps, spans, 2 * refl, 2 * band), F32),
            pltpu.VMEM((rows, X_SIZE * cut), BF16),
        ],
        flops=40 * eigen.size,
        size=12 * eigen.size,
        vmem=14,
    )


def piece_shapes(rows, cut):
    full, half = jax.ShapeDtypeStruct((rows, cut), BF16), jax.ShapeDtypeStruct((rows // 2, cut), BF16)
    return [full, full, full, half, half]


def traded(pieces):
    steps = (1, -1, 2) if len(pieces) == 4 else (1, -1, 2, -2)
    got = []
    for piece, step in zip(pieces[1:], steps):
        got.append(shifted(piece, "x", step))
    return got


def ring(block, far):
    ahead = behind = block
    found = [(0, block)]
    for step in range(1, Z_SIZE // 2):
        ahead = shifted(ahead, "z", 1)
        behind = shifted(behind, "z", -1)
        found += [(step, ahead), (Z_SIZE - step, behind)]
    found.append((Z_SIZE // 2, shifted(ahead if far > 0 else behind, "z", far)))
    return found


def products_kernel(*refs, spots, own, rows):
    blocks, (mine, one, two, half0, half1) = refs[: len(spots)], refs[len(spots) : len(spots) + 5]
    ordered_ref, sums_ref, eigen_ref = refs[len(spots) + 5 :]
    order = ordered_ref.shape[0]
    x, z = lax.axis_index("x"), lax.axis_index("z")
    for ref, units in zip(blocks, spots):
        for at, (back_z, back_x, panel) in enumerate(units):
            source = (x + X_SIZE - back_x) % X_SIZE * Z_SIZE + (z + Z_SIZE - back_z) % Z_SIZE
            to = pl.multiple_of(panel * (order // 2) + source * own, UNIT)
            ordered_ref[pl.ds(to, own), :] = ref[at * own : (at + 1) * own, :]
    sources = ((0, 0, mine), (1, 0, one), (3, 0, two), (2, 0, half0), (2, rows // 2, half1))
    for back, row, ref in sources:
        to = pl.multiple_of((x + X_SIZE - back) % X_SIZE * rows + row, UNIT)
        eigen_ref[pl.ds(to, ref.shape[0]), :] = ref[...]

    def put(value, at):
        sums_ref[at * LANE : (at + 1) * LANE] = value.astype(BF16)

    def dot(first, count, other):
        return lax.dot_general(
            ordered_ref[first : first + count, :], other, CONTRACT_LAST, preferred_element_type=F32
        )

    width = order // 2
    early = dot(0, order, ordered_ref[0:width, :])
    late = dot(width, width, ordered_ref[width:, :])
    inner = dot(0, order, eigen_ref[...])
    tile = lambda value, i, j: value[i * LANE : (i + 1) * LANE, j * LANE : (j + 1) * LANE]
    for i in range(4):
        put(tile(inner, i, 0), i)
    for at, (i, j) in enumerate(((0, 0), (0, 1), (1, 1), (2, 0), (2, 1), (3, 0), (3, 1))):
        put(tile(early, i, j), 4 + at)
    for at, (i, j) in enumerate(((0, 0), (0, 1), (1, 1))):
        put(tile(late, i, j), 11 + at)


TILES = {
    at: 4 + k
    for k, at in enumerate(
        ((0, 0), (0, 1), (1, 1), (2, 0), (2, 1), (3, 0), (3, 1), (2, 2), (2, 3), (3, 3))
    )
}


def products(found, pieces, spots, own, order, rows):
    cut = pieces[0].shape[1]
    return call(
        functools.partial(products_kernel, spots=spots, own=own, rows=rows),
        [
            jax.ShapeDtypeStruct((order, cut), BF16),
            jax.ShapeDtypeStruct(((4 + len(TILES)) * LANE, LANE), BF16),
        ],
        [VM] * (len(found) + len(pieces)),
        (*found, *pieces),
        [pltpu.VMEM((LANE, cut), BF16)],
        flops=2 * order * (order + LANE) * cut,
        size=6 * order * cut,
        vmem=18,
    )


def split(value):
    high = value.astype(BF16)
    return high, (value - high.astype(F32)).astype(BF16)


def fine_dot(a, b):
    a0, a1 = a if isinstance(a, tuple) else split(a)
    b0, b1 = b if isinstance(b, tuple) else split(b)
    dot = functools.partial(jnp.dot, preferred_element_type=F32)
    total = dot(a0, b0)
    if b1 is not None:
        total = total + dot(a0, b1)
    if a1 is not None:
        total = total + dot(a1, b0)
    return total


def small_inverses(grams):
    order = grams[0].shape[0]
    row = lax.broadcasted_iota(jnp.int32, (order, order), 0)
    col = lax.broadcasted_iota(jnp.int32, (order, order), 1)
    eye = row == col
    wide = [gram.astype(F32) for gram in grams]
    found = [jnp.where(eye, 2.0 / jnp.where(eye, gram, 1.0), 0.0) for gram in wide]
    size = 1
    while size < order:
        pick = (row // (2 * size) == col // (2 * size)) & (row // size < col // size)
        parts = [jnp.where(pick, gram, 0.0) for gram in wide]
        if size == 1:
            steps = [
                jnp.sum(f, axis=1, keepdims=True) * part * jnp.sum(f, axis=0, keepdims=True)
                for f, part in zip(found, parts)
            ]
        else:
            halves = [split(f) for f in found]
            steps = [fine_dot((part.astype(BF16), None), f) for part, f in zip(parts, halves)]
            steps = [fine_dot(f, step) for f, step in zip(halves, steps)]
        found = [f - step for f, step in zip(found, steps)]
        size *= 2
    return found


def correction_kernel(
    sums_ref, ordered_ref, mine_ref, next_ref, last_ref, one_ref, two_ref, coeffs_ref
):
    rows = mine_ref.shape[0]
    tile = lambda at: sums_ref[at * LANE : (at + 1) * LANE, :]
    gram = lambda i, j: tile(TILES[i, j])
    inverses = [split(f) for f in small_inverses([gram(i, i) for i in range(4)])]
    above = [
        split(fine_dot(inverses[at], fine_dot((gram(at, at + 1), None), inverses[at + 1])))
        for at in (0, 2)
    ]

    def solve(panel, first, second):
        at = 2 * panel
        return [
            fine_dot(inverses[at], first) - fine_dot(above[panel], second),
            fine_dot(inverses[at + 1], second),
        ]

    solved = solve(0, (tile(0), None), (tile(1), None))
    known = [value.astype(BF16) for value in solved]
    rest = [
        tile(i).astype(F32)
        - jnp.dot(gram(i, 0), known[0], preferred_element_type=F32)
        - jnp.dot(gram(i, 1), known[1], preferred_element_type=F32)
        for i in (2, 3)
    ]
    solved += solve(1, *map(split, rest))
    for i in range(4):
        turned = solved[i].T.astype(BF16)
        for x in range(X_SIZE):
            to = pl.multiple_of((x + X_SIZE - lax.axis_index("x")) % X_SIZE * rows, UNIT)
            coeffs_ref[pl.ds(to, rows), i * LANE : (i + 1) * LANE] = turned[x * rows : (x + 1) * rows]
    product = jnp.dot(
        coeffs_ref[...], ordered_ref[...], preferred_element_type=F32
    ).astype(BF16)
    piece = lambda step: product[step * rows : (step + 1) * rows]
    mine_ref[...] = piece(0)
    next_ref[...] = piece(PEERS[0])
    last_ref[...] = piece(PEERS[1])
    one_ref[...] = piece(PEERS[2])[0 : rows // 2]
    two_ref[...] = piece(PEERS[2])[rows // 2 :]


def correction(sums, ordered, rows):
    order, cut = ordered.shape
    return call(
        correction_kernel,
        piece_shapes(rows, cut),
        [VM, VM],
        (sums, ordered),
        [pltpu.VMEM((LANE, order), BF16)],
        flops=2 * order * LANE * cut,
        size=4 * order * cut,
        vmem=24,
    )


def subtract_kernel(eigen_ref, mine, one, two, half0, half1, out_ref, held_ref, sems):
    rows, columns = eigen_ref.shape
    cut = mine.shape[1]
    half = rows // 2
    sources = {0: ((0, mine),), 1: ((0, one),), 3: ((0, two),), 2: ((0, half0), (half, half1))}
    leaves = []
    for at in range(X_SIZE):
        begin, span = at * cut, min(cut, columns - at * cut)
        for back, refs in sources.items():

            @pl.when((lax.axis_index("x") + X_SIZE - back) % X_SIZE == at)
            def _(refs=refs, begin=begin, span=span):
                for row, ref in refs:
                    high = row + ref.shape[0]
                    held_ref[row:high, begin : begin + span] = (
                        eigen_ref[row:high, begin : begin + span] - ref[:, 0:span].astype(F32)
                    )

        chunk = slice(begin, begin + span)
        leaves.append(
            pltpu.make_async_copy(held_ref.at[:, chunk], out_ref.at[:, chunk], sems.at[at])
        )
        leaves[-1].start()
    for leave in leaves:
        leave.wait()


def subtract(eigen, pieces):
    return call(
        subtract_kernel,
        jax.ShapeDtypeStruct(eigen.shape, F32),
        [VM] * 6,
        (eigen, *pieces),
        [pltpu.VMEM(eigen.shape, F32), pltpu.SemaphoreType.DMA((X_SIZE,))],
        flops=eigen.size,
        size=10 * eigen.size,
        vmem=12,
        outs=ANY,
    )


def total_kernel(parts_ref, out_ref):
    total = parts_ref[0].astype(F32)
    for at in range(1, parts_ref.shape[0]):
        total = total + parts_ref[at].astype(F32)
    total = total.astype(BF16)
    for at in range(parts_ref.shape[0]):
        out_ref[at] = total


def total_for_all(parts):
    return call(
        total_kernel,
        jax.ShapeDtypeStruct(parts.shape, BF16),
        [VM],
        (parts,),
        flops=parts.size,
        size=4 * parts.size,
        vmem=4,
    )


def exchange(pieces, axes):
    return lax.all_to_all(pieces, axes, 0, 0, tiled=True)


def inner(eigvecs, span_vectors, span_offsets, panels):
    assert (lax.axis_size("x"), lax.axis_size("z")) == (X_SIZE, Z_SIZE)
    peers = lax.axis_size(ROW) * X_SIZE
    count, own, columns = panels.shape
    rows = eigvecs.shape[0]
    order = count * own * X_SIZE * Z_SIZE
    cut = -(-columns // (LANE * X_SIZE)) * LANE
    *packed, down, up = front(eigvecs, span_vectors, span_offsets, panels, cut)
    swept = sweep_all(eigvecs, span_vectors, span_offsets, down, up, cut)
    eigen, pieces = swept[0], swept[1:]
    one, two, far = traded(packed)
    found, spots = [], []
    for at, (pair, sources) in enumerate((((packed[0], one), (0, 1)), ((two, far), (3, 2)))):
        unit = [(back_x, panel) for back_x in sources for panel in range(count)]
        for back, block in ring(jnp.concatenate(pair, axis=0), 1 - 2 * at):
            found.append(block)
            spots.append([(back, back_x, panel) for back_x, panel in unit])
    others = [pieces[0], *traded(pieces)]
    ordered, sums = products(found, others, spots, own, order, rows)

    parts = exchange(sums.reshape(peers, -1, LANE), SUM_AXES)
    sums = exchange(total_for_all(parts), SUM_AXES)
    corrections = correction(sums.reshape(-1, LANE), ordered, rows)
    return subtract(eigen, [corrections[0], *traded(corrections)])


def solution(mesh):
    finer = Mesh(
        mesh.devices.reshape(mesh.shape["row"] // 2, 2, X_SIZE, Z_SIZE), (*ROW, *COL)
    )
    placed = (P(COL, ROW), P(None, ROW, None, None), P(None, ROW), P(None, COL, ROW))
    return jax.shard_map(inner, mesh=finer, in_specs=placed, out_specs=P(COL, ROW), check_vma=False)
```

```python
import functools

import jax
import jax.numpy as jnp
from jax import lax
from jax.experimental import pallas as pl
from jax.experimental.pallas import tpu as pltpu
from jax.sharding import Mesh
from jax.sharding import PartitionSpec as P


COL = ("x", "z")
ROW = ("y", "core")
SUM_AXES = ("y", "x", "core")
X_SIZE, Z_SIZE = 4, 8
LANE = 128
GROUP = 4
FRONT_MB = 60
UNIT = 8
F32 = jnp.float32
BF16 = jnp.bfloat16
CONTRACT_LAST = (((1,), (1,)), ((), ()))
VM = pl.BlockSpec(memory_space=pltpu.VMEM)
SM = pl.BlockSpec(memory_space=pltpu.SMEM)
ANY = pl.BlockSpec(memory_space=pl.ANY)
PEERS = (1, 3, 2)


def call(kernel, out_shape, in_specs, args, scratch=(), flops=0, size=0, vmem=0, outs=None):
    outs = outs or jax.tree.map(lambda _: VM, out_shape)
    return pl.pallas_call(
        kernel,
        out_shape=out_shape,
        in_specs=in_specs,
        out_specs=outs,
        scratch_shapes=list(scratch),
        compiler_params=pltpu.CompilerParams(vmem_limit_bytes=vmem << 20) if vmem else None,
        cost_estimate=pl.CostEstimate(flops=flops, bytes_accessed=size, transcendentals=0),
    )(*args)


def shifted(value, axis, steps):
    count = lax.axis_size(axis)
    return lax.ppermute(value, axis, [(at, (at + steps) % count) for at in range(count)])


def from_behind(value, axis, steps):
    count = lax.axis_size(axis)
    first, last = (max(0, -steps), min(count, count - steps))
    return lax.ppermute(value, axis, [(source, source + steps) for source in range(first, last)])


def span_factors(vectors):
    solved = []
    for i in range(len(vectors)):
        value = vectors[i]
        for j in range(i):
            value = value - jnp.sum(vectors[j] * vectors[i], axis=1, keepdims=True) * solved[j]
        pivot = 0.5 * jnp.sum(vectors[i] * vectors[i], axis=1, keepdims=True)
        solved.append(value / pivot)
    return solved


def lay_pairs(vectors, pairs_ref):
    refl, (spans, band) = len(vectors), vectors[0].shape
    factors = span_factors(vectors)
    for i in range(refl):
        pairs_ref[:, i, 0:band] = vectors[i]
        pairs_ref[:, refl + i, 0:band] = factors[i]
        pairs_ref[:, i, band:] = jnp.zeros((spans, band), F32)
        pairs_ref[:, refl + i, band:] = jnp.zeros((spans, band), F32)


def window_of(begin, width):
    return pl.ds(pl.multiple_of(begin // LANE * LANE, LANE), width)


def apply_spans(begins, pairs, state_ref):
    refl, width = pairs[0].shape[0] // 2, pairs[0].shape[1]
    moved = [pltpu.roll(pair, begin % LANE, 1) for begin, pair in zip(begins, pairs)]
    windows = [state_ref[:, window_of(begin, width)] for begin in begins]
    inner = [
        [jnp.sum(window * pair[i : i + 1, :], axis=1, keepdims=True) for i in range(refl)]
        for window, pair in zip(windows, moved)
    ]
    for begin, window, pair, sums in zip(begins, windows, moved, inner):
        for i in range(refl):
            window = window - sums[i] * pair[refl + i : refl + i + 1, :]
        state_ref[:, window_of(begin, width)] = window


def apply_span(begin, pair, state_ref):
    apply_spans([begin], [pair], state_ref)


def apply_in_order(begins, pairs_ref, spots, state_ref):
    if len(begins) == 1:
        apply_span(begins[0], pairs_ref[spots[0]], state_ref)
        return
    tiles = [begin // LANE for begin in begins]
    apart = [
        jnp.abs(one - other) >= pairs_ref.shape[-1] // LANE
        for at, one in enumerate(tiles)
        for other in tiles[:at]
    ]
    clear = functools.reduce(jnp.logical_and, apart)

    @pl.when(clear)
    def _():
        apply_spans(begins, [pairs_ref[spot] for spot in spots], state_ref)

    @pl.when(jnp.logical_not(clear))
    def _():
        half = len(begins) // 2
        apply_in_order(begins[:half], pairs_ref, spots[:half], state_ref)
        apply_in_order(begins[half:], pairs_ref, spots[half:], state_ref)


def front_kernel(
    offsets_ref, vectors_ref, panels_ref, eigen_ref, *refs
):
    *piece_refs, down_out, up_out = refs[:6]
    down_ref, up_ref, wide_ref, held_vectors_ref, held_offsets_ref, sems = refs[6:]
    sweeps, spans, refl, band = vectors_ref.shape
    rows, columns = eigen_ref.shape
    panels, own, _ = panels_ref.shape
    moves = [
        pltpu.make_async_copy(
            panels_ref.at[p], wide_ref.at[p * own : (p + 1) * own, 0:columns], sems.at[p]
        )
        for p in range(panels)
    ]
    halos = ((down_ref, None, sweeps), (up_ref, 0, sweeps - 1))
    for ref, begin, count in halos:
        width = ref.shape[1] - count * band - LANE
        begin = columns - width if begin is None else begin
        moves.append(
            pltpu.make_async_copy(
                eigen_ref.at[:, begin : begin + width], ref.at[:, 0:width], sems.at[len(moves)]
            )
        )
    small = [
        pltpu.make_async_copy(vectors_ref, held_vectors_ref, sems.at[len(moves)]),
        pltpu.make_async_copy(offsets_ref, held_offsets_ref, sems.at[len(moves) + 1]),
    ]
    for move in moves + small:
        move.start()
    wide_ref[:, columns:] = jnp.zeros((panels * own, wide_ref.shape[1] - columns), BF16)
    leaves = []

    def leave(source, target):
        leaves.append(pltpu.make_async_copy(source, target, sems.at[len(moves) + 2 + len(leaves)]))
        leaves[-1].start()

    for move in moves[:panels]:
        move.wait()
    for step, ref in zip((*PEERS, 0), (*piece_refs[1:], piece_refs[0])):
        cut = ref.shape[1]
        at = pl.multiple_of((lax.axis_index("x") + step) % X_SIZE * cut, LANE)
        leave(wide_ref.at[:, pl.ds(at, cut)], ref)
    for move in small:
        move.wait()
    for ref, _, count in halos:
        width = ref.shape[1] - count * band - LANE
        for sweep in range(count):
            for i in range(refl):
                ref[i * spans : (i + 1) * spans, width + sweep * band : width + (sweep + 1) * band] = (
                    held_vectors_ref[sweep, :, i, :]
                )
        ref[:, width + count * band :] = jnp.zeros((rows, LANE), F32)
        starts = held_offsets_ref[...].astype(F32)
        ref[0:sweeps, width + count * band : width + count * band + spans] = starts
    for move, source, target in zip(moves[panels:], (down_ref, up_ref), (down_out, up_out)):
        move.wait()
        leave(source, target)
    for move in leaves:
        move.wait()


def halo_sizes(vectors):
    sweeps, spans, _, band = vectors.shape
    return sweeps * spans * band, ((sweeps - 1) * spans + 1) * band


def front(eigen, vectors, offsets, panels, cut):
    sweeps, _, _, band = vectors.shape
    rows = eigen.shape[0]
    left, right = halo_sizes(vectors)
    wide = lambda width: jax.ShapeDtypeStruct((rows, width), F32)
    high = panels.shape[0] * panels.shape[1]
    return call(
        front_kernel,
        [jax.ShapeDtypeStruct((high, cut), BF16)] * 4
        + [wide(left + sweeps * band + LANE), wide(right + (sweeps - 1) * band + LANE)],
        [ANY] * 4,
        (offsets, vectors, panels, eigen),
        [
            pltpu.VMEM((rows, left + sweeps * band + LANE), F32),
            pltpu.VMEM((rows, right + (sweeps - 1) * band + LANE), F32),
            pltpu.VMEM((high, X_SIZE * cut), BF16),
            pltpu.VMEM(vectors.shape, F32),
            pltpu.VMEM(offsets.shape, jnp.int32),
            pltpu.SemaphoreType.DMA((panels.shape[0] + 10,)),
        ],
        flops=panels.size,
        size=4 * panels.size,
        vmem=FRONT_MB,
        outs=[ANY] * 6,
    )


def sweep_kernel(
    offsets_ref, upper_offsets_ref, lower_offsets_ref,
    vectors_ref, own_ref, upper_ref, lower_ref,
    out_ref, mine_ref, next_ref, last_ref, far_ref,
    state_ref, pairs_ref, rounded_ref,
):
    sweeps, spans, refl, band = vectors_ref.shape
    rows, columns = own_ref.shape
    left = upper_ref.shape[1] - sweeps * band - LANE
    right = lower_ref.shape[1] - (sweeps - 1) * band - LANE
    state_ref[:, 0:left] = upper_ref[:, 0:left]
    state_ref[:, left : left + columns] = own_ref[...]
    state_ref[:, left + columns :] = lower_ref[:, 0:right]
    first = lax.axis_index(ROW) == 0
    final = lax.axis_index(ROW) == lax.axis_size(ROW) - 1

    def beside(ref, width, sweep, i):
        return ref[i * spans : (i + 1) * spans, width + sweep * band : width + (sweep + 1) * band]

    for sweep in range(sweeps):
        lay_pairs([beside(upper_ref, left, sweep, i) for i in range(refl)], pairs_ref.at[sweep * 3])
        lay_pairs([vectors_ref[sweep, :, i, :] for i in range(refl)], pairs_ref.at[sweep * 3 + 1])
        if sweep < sweeps - 1:
            lay_pairs([beside(lower_ref, right, sweep, i) for i in range(refl)], pairs_ref.at[sweep * 3 + 2])
    for sweep in range(sweeps):

        def from_upper(at, carry, sweep=sweep):
            begin = upper_offsets_ref[sweep, at] - (columns - left)

            @pl.when(jnp.logical_and(begin >= 0, jnp.logical_not(first)))
            def _():
                apply_span(begin, pairs_ref[sweep * 3, at], state_ref)

            return carry

        def from_lower(at, carry, sweep=sweep):
            begin = lower_offsets_ref[sweep, at]

            @pl.when(jnp.logical_and(begin <= right - band, jnp.logical_not(final)))
            def _():
                apply_span(left + columns + begin, pairs_ref[sweep * 3 + 2, at], state_ref)

            return carry

        lax.fori_loop(0, spans, from_upper, 0)
        for at in range(0, spans, GROUP):
            group = range(at, at + GROUP)
            apply_in_order(
                [left + offsets_ref[sweep, k] for k in group],
                pairs_ref,
                [(sweep * 3 + 1, k) for k in group],
                state_ref,
            )
        if sweep < sweeps - 1:
            lax.fori_loop(0, spans, from_lower, 0)
    out_ref[...] = state_ref[:, left : left + columns]
    padded = rounded_ref.shape[1]
    rounded_ref[:, 0:columns] = state_ref[:, left : left + columns].astype(BF16)
    rounded_ref[:, columns:] = jnp.zeros((rows, padded - columns), BF16)
    cut = mine_ref.shape[1]
    targets = (
        (0, 0, mine_ref), (PEERS[0], 0, next_ref), (PEERS[1], 0, last_ref),
        (PEERS[2], 0, far_ref),
    )
    for step, row, ref in targets:
        at = pl.multiple_of((lax.axis_index("x") + step) % X_SIZE * cut, LANE)
        ref[...] = rounded_ref[row : row + ref.shape[0], pl.ds(at, cut)]


def sweep_all(eigen, vectors, offsets, down, up, cut):
    sweeps, spans, refl, band = vectors.shape
    rows, columns = eigen.shape
    left, right = halo_sizes(vectors)
    assert left + right + band < columns and spans * refl == rows
    upper = from_behind(down, ROW, 1)
    lower = from_behind(up, ROW, -1)
    upper_offsets = upper[0:sweeps, -LANE : spans - LANE].astype(jnp.int32)
    lower_offsets = lower[0:sweeps, -LANE : spans - LANE].astype(jnp.int32)
    return call(
        sweep_kernel,
        [jax.ShapeDtypeStruct(eigen.shape, F32)]
        + [jax.ShapeDtypeStruct((rows, cut), BF16)] * 4,
        [SM] * 3 + [VM] * 4,
        (offsets, upper_offsets, lower_offsets, vectors, eigen, upper, lower),
        [
            pltpu.VMEM((rows, left + columns + right), F32),
            pltpu.VMEM((3 * sweeps, spans, 2 * refl, 2 * band), F32),
            pltpu.VMEM((rows, X_SIZE * cut), BF16),
        ],
        flops=40 * eigen.size,
        size=12 * eigen.size,
        vmem=14,
    )


def piece_shapes(rows, cut):
    full, half = jax.ShapeDtypeStruct((rows, cut), BF16), jax.ShapeDtypeStruct((rows // 2, cut), BF16)
    return [full, full, full, half, half]


def traded(pieces):
    steps = (1, -1, 2) if len(pieces) == 4 else (1, -1, 2, -2)
    got = []
    for piece, step in zip(pieces[1:], steps):
        got.append(shifted(piece, "x", step))
    return got


def ring(block, far):
    ahead = behind = block
    found = [(0, block)]
    for step in range(1, Z_SIZE // 2):
        ahead = shifted(ahead, "z", 1)
        behind = shifted(behind, "z", -1)
        found += [(step, ahead), (Z_SIZE - step, behind)]
    found.append((Z_SIZE // 2, shifted(ahead if far > 0 else behind, "z", far)))
    return found


def products_kernel(*refs, spots, own, rows):
    blocks, (mine, one, two, far) = refs[: len(spots)], refs[len(spots) : len(spots) + 4]
    ordered_ref, sums_ref, eigen_ref = refs[len(spots) + 4 :]
    order = ordered_ref.shape[0]
    x, z = lax.axis_index("x"), lax.axis_index("z")
    for ref, units in zip(blocks, spots):
        for at, (back_z, back_x, panel) in enumerate(units):
            source = (x + X_SIZE - back_x) % X_SIZE * Z_SIZE + (z + Z_SIZE - back_z) % Z_SIZE
            to = pl.multiple_of(panel * (order // 2) + source * own, UNIT)
            ordered_ref[pl.ds(to, own), :] = ref[at * own : (at + 1) * own, :]
    sources = ((0, 0, mine), (1, 0, one), (3, 0, two), (2, 0, far))
    for back, row, ref in sources:
        to = pl.multiple_of((x + X_SIZE - back) % X_SIZE * rows + row, UNIT)
        eigen_ref[pl.ds(to, ref.shape[0]), :] = ref[...]

    def put(value, at):
        sums_ref[at * LANE : (at + 1) * LANE] = value.astype(BF16)

    def dot(first, count, other):
        return lax.dot_general(
            ordered_ref[first : first + count, :], other, CONTRACT_LAST, preferred_element_type=F32
        )

    width = order // 2
    early = dot(0, order, ordered_ref[0:width, :])
    late = dot(width, width, ordered_ref[width:, :])
    inner = dot(0, order, eigen_ref[...])
    tile = lambda value, i, j: value[i * LANE : (i + 1) * LANE, j * LANE : (j + 1) * LANE]
    for i in range(4):
        put(tile(inner, i, 0), i)
    for at, (i, j) in enumerate(((0, 0), (0, 1), (1, 1), (2, 0), (2, 1), (3, 0), (3, 1))):
        put(tile(early, i, j), 4 + at)
    for at, (i, j) in enumerate(((0, 0), (0, 1), (1, 1))):
        put(tile(late, i, j), 11 + at)


TILES = {
    at: 4 + k
    for k, at in enumerate(
        ((0, 0), (0, 1), (1, 1), (2, 0), (2, 1), (3, 0), (3, 1), (2, 2), (2, 3), (3, 3))
    )
}


def products(found, pieces, spots, own, order, rows):
    cut = pieces[0].shape[1]
    return call(
        functools.partial(products_kernel, spots=spots, own=own, rows=rows),
        [
            jax.ShapeDtypeStruct((order, cut), BF16),
            jax.ShapeDtypeStruct(((4 + len(TILES)) * LANE, LANE), BF16),
        ],
        [VM] * (len(found) + len(pieces)),
        (*found, *pieces),
        [pltpu.VMEM((LANE, cut), BF16)],
        flops=2 * order * (order + LANE) * cut,
        size=6 * order * cut,
        vmem=18,
    )


def split(value):
    high = value.astype(BF16)
    return high, (value - high.astype(F32)).astype(BF16)


def fine_dot(a, b):
    a0, a1 = a if isinstance(a, tuple) else split(a)
    b0, b1 = b if isinstance(b, tuple) else split(b)
    dot = functools.partial(jnp.dot, preferred_element_type=F32)
    total = dot(a0, b0)
    if b1 is not None:
        total = total + dot(a0, b1)
    if a1 is not None:
        total = total + dot(a1, b0)
    return total


def small_inverses(grams):
    order = grams[0].shape[0]
    row = lax.broadcasted_iota(jnp.int32, (order, order), 0)
    col = lax.broadcasted_iota(jnp.int32, (order, order), 1)
    eye = row == col
    wide = [gram.astype(F32) for gram in grams]
    found = [jnp.where(eye, 2.0 / jnp.where(eye, gram, 1.0), 0.0) for gram in wide]
    size = 1
    while size < order:
        pick = (row // (2 * size) == col // (2 * size)) & (row // size < col // size)
        parts = [jnp.where(pick, gram, 0.0) for gram in wide]
        if size == 1:
            steps = [
                jnp.sum(f, axis=1, keepdims=True) * part * jnp.sum(f, axis=0, keepdims=True)
                for f, part in zip(found, parts)
            ]
        else:
            halves = [split(f) for f in found]
            steps = [fine_dot((part.astype(BF16), None), f) for part, f in zip(parts, halves)]
            steps = [fine_dot(f, step) for f, step in zip(halves, steps)]
        found = [f - step for f, step in zip(found, steps)]
        size *= 2
    return found


def correction_kernel(
    sums_ref, ordered_ref, mine_ref, next_ref, last_ref, one_ref, two_ref, coeffs_ref
):
    rows = mine_ref.shape[0]
    tile = lambda at: sums_ref[at * LANE : (at + 1) * LANE, :]
    gram = lambda i, j: tile(TILES[i, j])
    inverses = [split(f) for f in small_inverses([gram(i, i) for i in range(4)])]
    above = [
        split(fine_dot(inverses[at], fine_dot((gram(at, at + 1), None), inverses[at + 1])))
        for at in (0, 2)
    ]

    def solve(panel, first, second):
        at = 2 * panel
        return [
            fine_dot(inverses[at], first) - fine_dot(above[panel], second),
            fine_dot(inverses[at + 1], second),
        ]

    solved = solve(0, (tile(0), None), (tile(1), None))
    known = [value.astype(BF16) for value in solved]
    rest = [
        tile(i).astype(F32)
        - jnp.dot(gram(i, 0), known[0], preferred_element_type=F32)
        - jnp.dot(gram(i, 1), known[1], preferred_element_type=F32)
        for i in (2, 3)
    ]
    solved += solve(1, *map(split, rest))
    for i in range(4):
        turned = solved[i].T.astype(BF16)
        for x in range(X_SIZE):
            to = pl.multiple_of((x + X_SIZE - lax.axis_index("x")) % X_SIZE * rows, UNIT)
            coeffs_ref[pl.ds(to, rows), i * LANE : (i + 1) * LANE] = turned[x * rows : (x + 1) * rows]
    product = jnp.dot(
        coeffs_ref[...], ordered_ref[...], preferred_element_type=F32
    ).astype(BF16)
    piece = lambda step: product[step * rows : (step + 1) * rows]
    mine_ref[...] = piece(0)
    next_ref[...] = piece(PEERS[0])
    last_ref[...] = piece(PEERS[1])
    one_ref[...] = piece(PEERS[2])[0 : rows // 2]
    two_ref[...] = piece(PEERS[2])[rows // 2 :]


def correction(sums, ordered, rows):
    order, cut = ordered.shape
    return call(
        correction_kernel,
        piece_shapes(rows, cut),
        [VM, VM],
        (sums, ordered),
        [pltpu.VMEM((LANE, order), BF16)],
        flops=2 * order * LANE * cut,
        size=4 * order * cut,
        vmem=24,
    )


def subtract_kernel(eigen_ref, mine, one, two, half0, half1, out_ref, held_ref, sems):
    rows, columns = eigen_ref.shape
    cut = mine.shape[1]
    half = rows // 2
    sources = {0: ((0, mine),), 1: ((0, one),), 3: ((0, two),), 2: ((0, half0), (half, half1))}
    leaves = []
    for at in range(X_SIZE):
        begin, span = at * cut, min(cut, columns - at * cut)
        for back, refs in sources.items():

            @pl.when((lax.axis_index("x") + X_SIZE - back) % X_SIZE == at)
            def _(refs=refs, begin=begin, span=span):
                for row, ref in refs:
                    high = row + ref.shape[0]
                    held_ref[row:high, begin : begin + span] = (
                        eigen_ref[row:high, begin : begin + span] - ref[:, 0:span].astype(F32)
                    )

        chunk = slice(begin, begin + span)
        leaves.append(
            pltpu.make_async_copy(held_ref.at[:, chunk], out_ref.at[:, chunk], sems.at[at])
        )
        leaves[-1].start()
    for leave in leaves:
        leave.wait()


def subtract(eigen, pieces):
    return call(
        subtract_kernel,
        jax.ShapeDtypeStruct(eigen.shape, F32),
        [VM] * 6,
        (eigen, *pieces),
        [pltpu.VMEM(eigen.shape, F32), pltpu.SemaphoreType.DMA((X_SIZE,))],
        flops=eigen.size,
        size=10 * eigen.size,
        vmem=12,
        outs=ANY,
    )


def total_kernel(parts_ref, out_ref):
    total = parts_ref[0].astype(F32)
    for at in range(1, parts_ref.shape[0]):
        total = total + parts_ref[at].astype(F32)
    total = total.astype(BF16)
    for at in range(parts_ref.shape[0]):
        out_ref[at] = total


def total_for_all(parts):
    return call(
        total_kernel,
        jax.ShapeDtypeStruct(parts.shape, BF16),
        [VM],
        (parts,),
        flops=parts.size,
        size=4 * parts.size,
        vmem=4,
    )


def exchange(pieces, axes):
    return lax.all_to_all(pieces, axes, 0, 0, tiled=True)


def inner(eigvecs, span_vectors, span_offsets, panels):
    assert (lax.axis_size("x"), lax.axis_size("z")) == (X_SIZE, Z_SIZE)
    peers = lax.axis_size(ROW) * X_SIZE
    count, own, columns = panels.shape
    rows = eigvecs.shape[0]
    order = count * own * X_SIZE * Z_SIZE
    cut = -(-columns // (LANE * X_SIZE)) * LANE
    *packed, down, up = front(eigvecs, span_vectors, span_offsets, panels, cut)
    swept = sweep_all(eigvecs, span_vectors, span_offsets, down, up, cut)
    eigen, pieces = swept[0], swept[1:]
    one, two, far = traded(packed)
    found, spots = [], []
    for at, (pair, sources) in enumerate((((packed[0], one), (0, 1)), ((two, far), (3, 2)))):
        unit = [(back_x, panel) for back_x in sources for panel in range(count)]
        for back, block in ring(jnp.concatenate(pair, axis=0), 1 - 2 * at):
            found.append(block)
            spots.append([(back, back_x, panel) for back_x, panel in unit])
    others = [pieces[0], *traded(pieces)]
    ordered, sums = products(found, others, spots, own, order, rows)

    parts = exchange(sums.reshape(peers, -1, LANE), SUM_AXES)
    sums = exchange(total_for_all(parts), SUM_AXES)
    corrections = correction(sums.reshape(-1, LANE), ordered, rows)
    return subtract(eigen, [corrections[0], *traded(corrections)])


def solution(mesh):
    finer = Mesh(
        mesh.devices.reshape(mesh.shape["row"] // 2, 2, X_SIZE, Z_SIZE), (*ROW, *COL)
    )
    placed = (P(COL, ROW), P(None, ROW, None, None), P(None, ROW), P(None, COL, ROW))
    return jax.shard_map(inner, mesh=finer, in_specs=placed, out_specs=P(COL, ROW), check_vma=False)
```
